32 devices in a mesh: data: 4 (over y, z), model: 8 (over x, core).
Axes of the slice: x: 4, y: 2, z: 2, core: 2. Of those that a mesh axis runs over, the one named last changes fastest.
The devices are a block of a 4x4x8 slice.
Arguments:
- hidden_in: bfloat16 [4, 2048, 2560], P('data', 'model'), parts along dimension 0
- seg_ids: int32 [4, 2048], P('data'), parts along dimension 0
- gain_attn: bfloat16 [2560], replicated
- w_qkv: bfloat16 [2560, 32, 3, 80], P(None, 'model')
- w_out: bfloat16 [32, 80, 2560], P('model')
- gain_mlp: bfloat16 [2560], replicated
- w_up: bfloat16 [2560, 10240], P(None, 'model')
- w_down: bfloat16 [10240, 2560], P('model')
- grad_out: bfloat16 [4, 2048, 2560], P('data', 'model'), parts along dimension 0
Outputs:
- output 1: bfloat16 [4, 2048, 2560], P('data', 'model'), parts along dimension 0
- output 2: bfloat16 [4, 2048, 2560], P('data', 'model'), parts along dimension 0
- output 3: bfloat16 [10240, 32, 3, 80], P('data', 'model'), parts along dimension 0
- output 4: bfloat16 [128, 80, 2560], P(('data', 'model')), parts along dimension 0
- output 5: bfloat16 [10240, 10240], P('data', 'model'), parts along dimension 0
- output 6: bfloat16 [40960, 2560], P(('data', 'model')), parts along dimension 0
- output 7: bfloat16 [10240], P('data'), parts along dimension 0
- output 8: bfloat16 [10240], P('data'), parts along dimension 0
There are 4 independent parts. The reference program is written for one: setup_inputs(seed, part) draws one part's arguments, and reference() takes and returns one part's arrays. A program takes and returns all parts, laid end to end along the dimension named above; an argument that names none is the same for every part.
All inputs are finite; a program needn't handle non-finite values.
Results may differ from the reference program's by a relative error of at most 0.02.
Values are sent between devices in bfloat16 or wider.
A program may use at most 768 MiB of HBM per device.

```python
import jax
import jax.numpy as jnp
from jax import lax

BATCH = 1
SEQ_LEN = 2048
HIDDEN = 2560
HEADS = 32
HEAD_DIM = 80
FFN_DIM = 10240

LN_EPS = 1e-5
TOKENS = BATCH * SEQ_LEN
QKV_WIDTH = 3 * HEADS * HEAD_DIM
ATTN_WIDTH = HEADS * HEAD_DIM


def draw_segments(seg_key):
    cut_points = jax.random.randint(seg_key, (BATCH, 3), 1, SEQ_LEN)
    positions = jnp.arange(SEQ_LEN)
    return jnp.sum(positions[None, :, None] >= cut_points[:, None, :], axis=-1).astype(jnp.int32)


def normal_array(rand_key, shape, scale):
    return (scale * jax.random.normal(rand_key, shape, jnp.float32)).astype(jnp.bfloat16)


def setup_inputs(seed: int = 0, part: int = 0) -> dict:
    root_key = jax.random.key(seed)
    shared = jax.random.split(root_key, 6)
    part_keys = jax.random.split(jax.random.fold_in(root_key, part), 3)
    return {
        'hidden_in': normal_array(part_keys[0], (BATCH, SEQ_LEN, HIDDEN), 1.0),
        'seg_ids': draw_segments(part_keys[2]),
        'gain_attn': (1.0 + 0.3 * jax.random.normal(shared[0], (HIDDEN,), jnp.float32)).astype(jnp.bfloat16),
        'w_qkv': normal_array(shared[2], (HIDDEN, HEADS, 3, HEAD_DIM), 1.5 * HIDDEN ** -0.5),
        'w_out': normal_array(shared[3], (HEADS, HEAD_DIM, HIDDEN), 1.5 * ATTN_WIDTH ** -0.5),
        'gain_mlp': (1.0 + 0.3 * jax.random.normal(shared[1], (HIDDEN,), jnp.float32)).astype(jnp.bfloat16),
        'w_up': normal_array(shared[4], (HIDDEN, FFN_DIM), HIDDEN ** -0.5),
        'w_down': normal_array(shared[5], (FFN_DIM, HIDDEN), FFN_DIM ** -0.5),
        'grad_out': normal_array(part_keys[1], (BATCH, SEQ_LEN, HIDDEN), 1.0),
    }


def layer_norm(x_f32, gain_f32):
    mean_val = jnp.mean(x_f32, axis=-1, keepdims=True)
    centered = x_f32 - mean_val
    variance = jnp.mean(centered * centered, axis=-1, keepdims=True)
    return centered * lax.rsqrt(variance + LN_EPS) * gain_f32


def gelu_tanh(pre_act):
    return jax.nn.gelu(pre_act, approximate=True)


def head_probs(q_head, k_head, attn_mask):
    scores = jnp.einsum('bqd,bkd->bqk', q_head.astype(jnp.float32), k_head.astype(jnp.float32)) * HEAD_DIM ** -0.5
    return jax.nn.softmax(jnp.where(attn_mask, scores, -1e30), axis=-1)


def head_forward(head_qkv, attn_mask):
    attn_prob = head_probs(head_qkv[0], head_qkv[1], attn_mask)
    prob_lo = attn_prob.astype(jnp.bfloat16).astype(jnp.float32)
    return jnp.einsum('bqk,bkd->bqd', prob_lo, head_qkv[2].astype(jnp.float32)).astype(jnp.bfloat16)


def head_backward(head_qkv, head_out, d_head, attn_mask):
    q_head = head_qkv[0].astype(jnp.float32)
    k_head = head_qkv[1].astype(jnp.float32)
    v_head = head_qkv[2].astype(jnp.float32)
    attn_prob = head_probs(head_qkv[0], head_qkv[1], attn_mask)
    d_out = d_head.astype(jnp.float32)
    d_prob = jnp.einsum('bqd,bkd->bqk', d_out, v_head)
    row_delta = jnp.sum(d_out * head_out.astype(jnp.float32), axis=-1, keepdims=True)
    d_scores = (attn_prob * (d_prob - row_delta) * HEAD_DIM ** -0.5).astype(jnp.bfloat16).astype(jnp.float32)
    d_q = jnp.einsum('bqk,bkd->bqd', d_scores, k_head).astype(jnp.bfloat16)
    d_k = jnp.einsum('bqk,bqd->bkd', d_scores, q_head).astype(jnp.bfloat16)
    prob_lo = attn_prob.astype(jnp.bfloat16).astype(jnp.float32)
    d_v = jnp.einsum('bqk,bqd->bkd', prob_lo, d_out).astype(jnp.bfloat16)
    return jnp.stack([d_q, d_k, d_v])


def reference(hidden_in, seg_ids, gain_attn, w_qkv, w_out, gain_mlp, w_up, w_down, grad_out):
    x_rows = hidden_in.reshape(TOKENS, HIDDEN).astype(jnp.float32)
    ln1_out, ln1_vjp = jax.vjp(layer_norm, x_rows, gain_attn.astype(jnp.float32))
    attn_in = ln1_out.astype(jnp.bfloat16)
    w_qkv_flat = w_qkv.reshape(HIDDEN, QKV_WIDTH)
    qkv_flat = jnp.dot(attn_in, w_qkv_flat, preferred_element_type=jnp.float32).astype(jnp.bfloat16)
    qkv_heads = jnp.transpose(qkv_flat.reshape(BATCH, SEQ_LEN, HEADS, 3, HEAD_DIM), (2, 3, 0, 1, 4))
    positions = jnp.arange(SEQ_LEN)
    attn_mask = (positions[None, :, None] >= positions[None, None, :]) & (seg_ids[:, :, None] == seg_ids[:, None, :])
    attn_heads = lax.map(lambda head_qkv: head_forward(head_qkv, attn_mask), qkv_heads)
    attn_cat = jnp.transpose(attn_heads, (1, 2, 0, 3)).reshape(TOKENS, ATTN_WIDTH)
    w_out_flat = w_out.reshape(ATTN_WIDTH, HIDDEN)
    attn_sum = jnp.dot(attn_cat, w_out_flat, preferred_element_type=jnp.float32).astype(jnp.bfloat16)
    mid_rows = (x_rows + attn_sum.astype(jnp.float32)).astype(jnp.bfloat16)
    ln2_out, ln2_vjp = jax.vjp(layer_norm, mid_rows.astype(jnp.float32), gain_mlp.astype(jnp.float32))
    mlp_in = ln2_out.astype(jnp.bfloat16)
    pre_act = jnp.dot(mlp_in, w_up, preferred_element_type=jnp.float32)
    act_f32, gelu_vjp = jax.vjp(gelu_tanh, pre_act)
    act_lo = act_f32.astype(jnp.bfloat16)
    mlp_sum = jnp.dot(act_lo, w_down, preferred_element_type=jnp.float32).astype(jnp.bfloat16)
    out_rows = (mid_rows.astype(jnp.float32) + mlp_sum.astype(jnp.float32)).astype(jnp.bfloat16)
    dy_rows = grad_out.reshape(TOKENS, HIDDEN)
    d_act = jnp.dot(dy_rows, w_down.T, preferred_element_type=jnp.float32)
    d_pre = gelu_vjp(d_act)[0].astype(jnp.bfloat16)
    g_down = jnp.dot(act_lo.T, dy_rows, preferred_element_type=jnp.float32).astype(jnp.bfloat16)
    d_mlp_in = jnp.dot(d_pre, w_up.T, preferred_element_type=jnp.float32).astype(jnp.bfloat16)
    g_up = jnp.dot(mlp_in.T, d_pre, preferred_element_type=jnp.float32).astype(jnp.bfloat16)
    d_mid_ln, d_gain_mlp = ln2_vjp(d_mlp_in.astype(jnp.float32))
    d_mid = (dy_rows.astype(jnp.float32) + d_mid_ln).astype(jnp.bfloat16)
    d_attn_cat = jnp.dot(d_mid, w_out_flat.T, preferred_element_type=jnp.float32).astype(jnp.bfloat16)
    g_out = jnp.dot(attn_cat.T, d_mid, preferred_element_type=jnp.float32).astype(jnp.bfloat16)
    d_heads = jnp.transpose(d_attn_cat.reshape(BATCH, SEQ_LEN, HEADS, HEAD_DIM), (2, 0, 1, 3))
    d_qkv_heads = lax.map(lambda head_args: head_backward(head_args[0], head_args[1], head_args[2], attn_mask), (qkv_heads, attn_heads, d_heads))
    d_qkv = jnp.transpose(d_qkv_heads, (2, 3, 0, 1, 4)).reshape(TOKENS, QKV_WIDTH)
    d_attn_in = jnp.dot(d_qkv, w_qkv_flat.T, preferred_element_type=jnp.float32).astype(jnp.bfloat16)
    g_qkv = jnp.dot(attn_in.T, d_qkv, preferred_element_type=jnp.float32).astype(jnp.bfloat16)
    d_x_ln, d_gain_attn = ln1_vjp(d_attn_in.astype(jnp.float32))
    grad_in = (d_mid.astype(jnp.float32) + d_x_ln).astype(jnp.bfloat16)
    return (out_rows.reshape(BATCH, SEQ_LEN, HIDDEN), grad_in.reshape(BATCH, SEQ_LEN, HIDDEN), g_qkv.reshape(HIDDEN, HEADS, 3, HEAD_DIM), g_out.reshape(HEADS, HEAD_DIM, HIDDEN), g_up, g_down, d_gain_attn.astype(jnp.bfloat16), d_gain_mlp.astype(jnp.bfloat16))
```

```python
import functools

import jax
import jax.numpy as jnp
from jax import lax
from jax.experimental import pallas as pl
from jax.experimental.pallas import tpu as pltpu
from jax.sharding import PartitionSpec as P

LN_EPS = 1e-5
BLK = 256
NT = (((1,), (1,)), ((), ()))


def layer_norm(x_f32, gain_f32):
    mean_val = jnp.mean(x_f32, axis=-1, keepdims=True)
    centered = x_f32 - mean_val
    variance = jnp.mean(centered * centered, axis=-1, keepdims=True)
    return centered * lax.rsqrt(variance + LN_EPS) * gain_f32


def gelu_tanh(pre_act):
    return jax.nn.gelu(pre_act, approximate=True)


def dot32(a, b):
    return jnp.dot(a, b, preferred_element_type=jnp.float32)


def visible(j, i, first_row):
    kpos = j * BLK + lax.broadcasted_iota(jnp.int32, (BLK, BLK), 0)
    qpos = i * BLK + lax.broadcasted_iota(jnp.int32, (BLK, BLK), 1)
    return (kpos <= qpos) & (kpos >= first_row)


def attn_fwd_kernel(heads, hd, lo_ref, qkv_ref, first_ref, o_ref, lse_ref, k_s, s_s, o_s):
    i = pl.program_id(0)
    scale = hd ** -0.5

    @pl.when(i == 0)
    def _():
        for h in range(heads):
            for j in range(k_s.shape[1] // BLK):
                kt = qkv_ref[(3 * h + 1) * hd:(3 * h + 2) * hd, j * BLK:(j + 1) * BLK]
                k_s[h, j * BLK:(j + 1) * BLK, :] = kt.T

    lo = lo_ref[i]
    cols = pl.ds(pl.multiple_of(i * BLK, BLK), BLK)
    first_row = first_ref[0:1, cols]
    neg = jnp.full((8, BLK), -jnp.inf, jnp.float32)

    def scores(j, m):
        rows = pl.ds(pl.multiple_of(j * BLK, BLK), BLK)
        mask = visible(j, i, first_row)
        out = []
        for h in range(heads):
            s = dot32(k_s[h, rows, :], qkv_ref[3 * h * hd:(3 * h + 1) * hd, cols]) * scale
            s = jnp.where(mask, s, -1e30)
            s_s[h, rows, :] = s
            out.append(jnp.maximum(m[h], jnp.max(s.reshape(BLK // 8, 8, BLK), axis=0)))
        return tuple(out)

    m = lax.fori_loop(lo, i + 1, scores, (neg,) * heads)
    m = [jnp.max(x, axis=0, keepdims=True) for x in m]

    def expo(j, l):
        rows = pl.ds(pl.multiple_of(j * BLK, BLK), BLK)
        out = []
        for h in range(heads):
            e = jnp.exp(s_s[h, rows, :] - m[h])
            s_s[h, rows, :] = e
            out.append(l[h] + jnp.sum(e.reshape(BLK // 8, 8, BLK), axis=0))
        return tuple(out)

    l = lax.fori_loop(lo, i + 1, expo, (jnp.zeros((8, BLK), jnp.float32),) * heads)
    l = [jnp.sum(x, axis=0, keepdims=True) for x in l]
    r = [1.0 / x for x in l]
    for h in range(heads):
        lse_ref[h:h + 1, :] = m[h] + jnp.log(l[h])
        o_s[h] = jnp.zeros((hd, BLK), jnp.float32)

    def values(j, c):
        rows = pl.ds(pl.multiple_of(j * BLK, BLK), BLK)
        for h in range(heads):
            pb = (s_s[h, rows, :] * r[h]).astype(jnp.bfloat16)
            o_s[h] += dot32(qkv_ref[(3 * h + 2) * hd:(3 * h + 3) * hd, rows], pb)
        return c

    lax.fori_loop(lo, i + 1, values, 0)
    for h in range(heads):
        o_ref[h * hd:(h + 1) * hd, :] = o_s[h].astype(jnp.bfloat16)


def attention_fwd(qkv_t, lo, first, heads, hd):
    seq = qkv_t.shape[1]
    nb = seq // BLK
    flops = 4 * heads * seq * seq * hd // 2
    return pl.pallas_call(
        functools.partial(attn_fwd_kernel, heads, hd),
        grid_spec=pltpu.PrefetchScalarGridSpec(
            num_scalar_prefetch=1, grid=(nb,),
            in_specs=[pl.BlockSpec(qkv_t.shape, lambda i, lo: (0, 0)),
                      pl.BlockSpec((1, seq), lambda i, lo: (0, 0))],
            out_specs=[pl.BlockSpec((heads * hd, BLK), lambda i, lo: (0, i)),
                       pl.BlockSpec((8, BLK), lambda i, lo: (0, i))],
            scratch_shapes=[pltpu.VMEM((heads, seq, hd), jnp.bfloat16),
                            pltpu.VMEM((heads, seq, BLK), jnp.float32),
                            pltpu.VMEM((heads, hd, BLK), jnp.float32)]),
        out_shape=[jax.ShapeDtypeStruct((heads * hd, seq), jnp.bfloat16),
                   jax.ShapeDtypeStruct((8, seq), jnp.float32)],
        compiler_params=pltpu.CompilerParams(vmem_limit_bytes=56 * 2 ** 20),
        cost_estimate=pl.CostEstimate(flops=8 * flops, bytes_accessed=2 * qkv_t.size, transcendentals=0),
        name="attn_fwd",
    )(lo, qkv_t, first)


def attn_bwd_kernel(heads, hd, lo_ref, qkv_ref, o_ref, do_ref, lse_ref, first_ref, d_ref,
                    k_s, v_s, dq_s, dk_s, dv_s):
    i = pl.program_id(0)
    seq = qkv_ref.shape[1]
    scale = hd ** -0.5

    @pl.when(i == 0)
    def _():
        dk_s[...] = jnp.zeros_like(dk_s)
        dv_s[...] = jnp.zeros_like(dv_s)
        for h in range(heads):
            for j in range(seq // BLK):
                c = slice(j * BLK, (j + 1) * BLK)
                k_s[h, c, :] = qkv_ref[(3 * h + 1) * hd:(3 * h + 2) * hd, c].T
                v_s[h, c, :] = qkv_ref[(3 * h + 2) * hd:(3 * h + 3) * hd, c].T

    lo = lo_ref[i]
    cols = pl.ds(pl.multiple_of(i * BLK, BLK), BLK)
    first_row = first_ref[0:1, cols]
    delta = []
    for h in range(heads):
        hs = slice(h * hd, (h + 1) * hd)
        delta.append(jnp.sum(do_ref[hs, :].astype(jnp.float32) * o_ref[hs, :].astype(jnp.float32), axis=0, keepdims=True))
        dq_s[h] = jnp.zeros((hd, BLK), jnp.float32)

    def step(j, c):
        rows = pl.ds(pl.multiple_of(j * BLK, BLK), BLK)
        mask = visible(j, i, first_row)
        for h in range(heads):
            q_t = qkv_ref[3 * h * hd:(3 * h + 1) * hd, cols]
            do_t = do_ref[h * hd:(h + 1) * hd, :]
            s = dot32(k_s[h, rows, :], q_t) * scale
            p = jnp.exp(jnp.where(mask, s, -1e30) - lse_ref[h:h + 1, :])
            dp = dot32(v_s[h, rows, :], do_t)
            ds = (p * (dp - delta[h]) * scale).astype(jnp.bfloat16)
            pb = p.astype(jnp.bfloat16)
            dq_s[h] += dot32(qkv_ref[(3 * h + 1) * hd:(3 * h + 2) * hd, rows], ds)
            dk_s[h, :, rows] += lax.dot_general(q_t, ds, NT, preferred_element_type=jnp.float32)
            dv_s[h, :, rows] += lax.dot_general(do_t, pb, NT, preferred_element_type=jnp.float32)
        return c

    lax.fori_loop(lo, i + 1, step, 0)
    for h in range(heads):
        d_ref[3 * h * hd:(3 * h + 1) * hd, cols] = dq_s[h].astype(jnp.bfloat16)

    @pl.when(i == pl.num_programs(0) - 1)
    def _():
        for h in range(heads):
            d_ref[(3 * h + 1) * hd:(3 * h + 2) * hd, :] = dk_s[h].astype(jnp.bfloat16)
            d_ref[(3 * h + 2) * hd:(3 * h + 3) * hd, :] = dv_s[h].astype(jnp.bfloat16)


def attention_bwd(qkv_t, o_t, do_t, lse, lo, first, heads, hd):
    seq = qkv_t.shape[1]
    nb = seq // BLK
    flops = 10 * heads * seq * seq * hd // 2
    blk = lambda rows: pl.BlockSpec((rows, BLK), lambda i, lo: (0, i))
    return pl.pallas_call(
        functools.partial(attn_bwd_kernel, heads, hd),
        grid_spec=pltpu.PrefetchScalarGridSpec(
            num_scalar_prefetch=1, grid=(nb,),
            in_specs=[pl.BlockSpec(qkv_t.shape, lambda i, lo: (0, 0)), blk(heads * hd), blk(heads * hd), blk(8),
                      pl.BlockSpec((1, seq), lambda i, lo: (0, 0))],
            out_specs=pl.BlockSpec(qkv_t.shape, lambda i, lo: (0, 0)),
            scratch_shapes=[pltpu.VMEM((heads, seq, hd), jnp.bfloat16),
                            pltpu.VMEM((heads, seq, hd), jnp.bfloat16),
                            pltpu.VMEM((heads, hd, BLK), jnp.float32),
                            pltpu.VMEM((heads, hd, seq), jnp.float32),
                            pltpu.VMEM((heads, hd, seq), jnp.float32)]),
        out_shape=jax.ShapeDtypeStruct(qkv_t.shape, jnp.bfloat16),
        compiler_params=pltpu.CompilerParams(vmem_limit_bytes=56 * 2 ** 20),
        cost_estimate=pl.CostEstimate(flops=8 * flops, bytes_accessed=4 * qkv_t.size, transcendentals=0),
        name="attn_bwd",
    )(lo, qkv_t, o_t, do_t, lse, first)


def group_sum(vals, n):
    total = vals
    for shift in range(1, n):
        total = total + lax.ppermute(vals, 'model', [(a, (a + shift) % n) for a in range(n)])
    return total


def local_layer(n, hidden_in, seg_ids, gain_attn, w_qkv, w_out, gain_mlp, w_up, w_down, grad_out):
    heads, hd, hidden = w_out.shape
    seq_len = seg_ids.shape[1]
    x_f32 = hidden_in[0].astype(jnp.float32)
    dy = grad_out[0]
    wq_t = jnp.transpose(w_qkv, (1, 2, 3, 0)).reshape(heads * 3 * hd, hidden)
    wo = w_out.reshape(heads * hd, hidden)
    first = jnp.sum(seg_ids[0][:, None] < seg_ids[0][None, :], axis=0, dtype=jnp.int32)
    lo = first[::BLK] // BLK
    first = first[None]
    ein = functools.partial(jnp.einsum, preferred_element_type=jnp.float32)
    gather = lambda a: lax.all_gather(a, 'model', axis=0, tiled=True)
    scatter = lambda a: lax.psum_scatter(a, 'model', scatter_dimension=0, tiled=True)

    ln1_out, ln1_vjp = jax.vjp(layer_norm, x_f32, gain_attn.astype(jnp.float32))
    attn_in = gather(ln1_out.astype(jnp.bfloat16))
    qkv_t = ein('nd,sd->ns', wq_t, attn_in).astype(jnp.bfloat16)
    o_t, lse = attention_fwd(qkv_t, lo, first, heads, hd)
    attn_sum = scatter(ein('es,ed->sd', o_t, wo).astype(jnp.bfloat16))
    mid_loc = (x_f32 + attn_sum.astype(jnp.float32)).astype(jnp.bfloat16)
    ln2_out, ln2_vjp = jax.vjp(layer_norm, mid_loc.astype(jnp.float32), gain_mlp.astype(jnp.float32))
    mlp_in = gather(ln2_out.astype(jnp.bfloat16))
    pre_act = ein('sd,df->sf', mlp_in, w_up)
    act_f32, gelu_vjp = jax.vjp(gelu_tanh, pre_act)
    act_lo = act_f32.astype(jnp.bfloat16)
    grad_full = gather(dy)
    d_act = ein('sd,fd->sf', grad_full, w_down)
    d_pre = gelu_vjp(d_act)[0].astype(jnp.bfloat16)
    d_mlp_in = scatter(ein('sf,df->sd', d_pre, w_up).astype(jnp.bfloat16))
    mlp_sum = scatter(ein('sf,fd->sd', act_lo, w_down).astype(jnp.bfloat16))
    hidden_out = (mid_loc.astype(jnp.float32) + mlp_sum.astype(jnp.float32)).astype(jnp.bfloat16)
    g_down = ein('sf,sd->fd', act_lo, grad_full).astype(jnp.bfloat16)
    g_up = ein('sd,sf->df', mlp_in, d_pre).astype(jnp.bfloat16)
    d_mid_ln, d_gain_mlp = ln2_vjp(d_mlp_in.astype(jnp.float32))
    d_mid = (dy.astype(jnp.float32) + d_mid_ln).astype(jnp.bfloat16)
    d_mid_full = gather(d_mid)
    do_t = ein('ed,sd->es', wo, d_mid_full).astype(jnp.bfloat16)
    g_out = ein('es,sd->ed', o_t, d_mid_full).astype(jnp.bfloat16)
    dqkv_t = attention_bwd(qkv_t, o_t, do_t, lse, lo, first, heads, hd)
    d_attn_in = scatter(ein('ns,nd->sd', dqkv_t, wq_t).astype(jnp.bfloat16))
    g_qkv = ein('ns,sd->nd', dqkv_t, attn_in).astype(jnp.bfloat16)
    d_x_ln, d_gain_attn = ln1_vjp(d_attn_in.astype(jnp.float32))
    grad_in = (d_mid.astype(jnp.float32) + d_x_ln).astype(jnp.bfloat16)
    gain_sums = group_sum(jnp.stack([d_gain_attn, d_gain_mlp]), n).astype(jnp.bfloat16)
    g_qkv = jnp.transpose(g_qkv.reshape(heads, 3, hd, hidden), (3, 0, 1, 2))
    return (hidden_out[None], grad_in[None], g_qkv, g_out.reshape(heads, hd, hidden), g_up, g_down,
            gain_sums[0], gain_sums[1])


def solution(mesh):
    act_spec = P('data', 'model', None)
    in_specs = (act_spec, P('data', None), P(), P(None, 'model', None, None), P('model', None, None), P(), P(None, 'model'), P('model', None), act_spec)
    out_specs = (act_spec, act_spec, P('data', 'model', None, None), P(('data', 'model'), None, None), P('data', 'model'), P(('data', 'model'), None), P('data'), P('data'))
    return jax.shard_map(functools.partial(local_layer, mesh.shape['model']), mesh=mesh, in_specs=in_specs, out_specs=out_specs, check_vma=False)
```

```python
import functools

import jax
import jax.numpy as jnp
from jax import lax
from jax.experimental import pallas as pl
from jax.experimental.pallas import tpu as pltpu
from jax.sharding import PartitionSpec as P

LN_EPS = 1e-5
BLK = 256
NT = (((1,), (1,)), ((), ()))
MESH = pl.DeviceIdType.MESH


def layer_norm(x_f32, gain_f32):
    mean_val = jnp.mean(x_f32, axis=-1, keepdims=True)
    centered = x_f32 - mean_val
    variance = jnp.mean(centered * centered, axis=-1, keepdims=True)
    return centered * lax.rsqrt(variance + LN_EPS) * gain_f32


def gelu_tanh(pre_act):
    return jax.nn.gelu(pre_act, approximate=True)


def dot32(a, b):
    return jnp.dot(a, b, preferred_element_type=jnp.float32)


def visible(j, i, first_row):
    kpos = j * BLK + lax.broadcasted_iota(jnp.int32, (BLK, BLK), 0)
    qpos = i * BLK + lax.broadcasted_iota(jnp.int32, (BLK, BLK), 1)
    return (kpos <= qpos) & (kpos >= first_row)


def attn_fwd_kernel(heads, hd, lo_ref, qkv_ref, first_ref, o_ref, lse_ref, k_s, s_s, o_s):
    i = pl.program_id(0)
    scale = hd ** -0.5

    @pl.when(i == 0)
    def _():
        for h in range(heads):
            for j in range(k_s.shape[1] // BLK):
                kt = qkv_ref[(3 * h + 1) * hd:(3 * h + 2) * hd, j * BLK:(j + 1) * BLK]
                k_s[h, j * BLK:(j + 1) * BLK, :] = kt.T

    lo = lo_ref[i]
    cols = pl.ds(pl.multiple_of(i * BLK, BLK), BLK)
    first_row = first_ref[0:1, cols]
    neg = jnp.full((8, BLK), -jnp.inf, jnp.float32)

    def scores(j, m):
        rows = pl.ds(pl.multiple_of(j * BLK, BLK), BLK)
        mask = visible(j, i, first_row)
        out = []
        for h in range(heads):
            s = dot32(k_s[h, rows, :], qkv_ref[3 * h * hd:(3 * h + 1) * hd, cols]) * scale
            s = jnp.where(mask, s, -1e30)
            s_s[h, rows, :] = s
            out.append(jnp.maximum(m[h], jnp.max(s.reshape(BLK // 8, 8, BLK), axis=0)))
        return tuple(out)

    m = lax.fori_loop(lo, i + 1, scores, (neg,) * heads)
    m = [jnp.max(x, axis=0, keepdims=True) for x in m]

    def expo(j, l):
        rows = pl.ds(pl.multiple_of(j * BLK, BLK), BLK)
        out = []
        for h in range(heads):
            e = jnp.exp(s_s[h, rows, :] - m[h])
            s_s[h, rows, :] = e
            out.append(l[h] + jnp.sum(e.reshape(BLK // 8, 8, BLK), axis=0))
        return tuple(out)

    l = lax.fori_loop(lo, i + 1, expo, (jnp.zeros((8, BLK), jnp.float32),) * heads)
    l = [jnp.sum(x, axis=0, keepdims=True) for x in l]
    r = [1.0 / x for x in l]
    for h in range(heads):
        lse_ref[h:h + 1, :] = m[h] + jnp.log(l[h])
        o_s[h] = jnp.zeros((hd, BLK), jnp.float32)

    def values(j, c):
        rows = pl.ds(pl.multiple_of(j * BLK, BLK), BLK)
        for h in range(heads):
            pb = (s_s[h, rows, :] * r[h]).astype(jnp.bfloat16)
            o_s[h] += dot32(qkv_ref[(3 * h + 2) * hd:(3 * h + 3) * hd, rows], pb)
        return c

    lax.fori_loop(lo, i + 1, values, 0)
    for h in range(heads):
        o_ref[h * hd:(h + 1) * hd, :] = o_s[h].astype(jnp.bfloat16)


def attention_fwd(qkv_t, lo, first, heads, hd):
    seq = qkv_t.shape[1]
    nb = seq // BLK
    flops = 4 * heads * seq * seq * hd // 2
    return pl.pallas_call(
        functools.partial(attn_fwd_kernel, heads, hd),
        grid_spec=pltpu.PrefetchScalarGridSpec(
            num_scalar_prefetch=1, grid=(nb,),
            in_specs=[pl.BlockSpec(qkv_t.shape, lambda i, lo: (0, 0)),
                      pl.BlockSpec((1, seq), lambda i, lo: (0, 0))],
            out_specs=[pl.BlockSpec((heads * hd, BLK), lambda i, lo: (0, i)),
                       pl.BlockSpec((8, BLK), lambda i, lo: (0, i))],
            scratch_shapes=[pltpu.VMEM((heads, seq, hd), jnp.bfloat16),
                            pltpu.VMEM((heads, seq, BLK), jnp.float32),
                            pltpu.VMEM((heads, hd, BLK), jnp.float32)]),
        out_shape=[jax.ShapeDtypeStruct((heads * hd, seq), jnp.bfloat16),
                   jax.ShapeDtypeStruct((8, seq), jnp.float32)],
        compiler_params=pltpu.CompilerParams(vmem_limit_bytes=56 * 2 ** 20),
        cost_estimate=pl.CostEstimate(flops=8 * flops, bytes_accessed=2 * qkv_t.size, transcendentals=0),
        name="attn_fwd",
    )(lo, qkv_t, first)


def attn_bwd_kernel(heads, hd, lo_ref, qkv_ref, o_ref, do_ref, lse_ref, first_ref, d_ref,
                    k_s, v_s, dq_s, dk_s, dv_s):
    i = pl.program_id(0)
    seq = qkv_ref.shape[1]
    scale = hd ** -0.5

    @pl.when(i == 0)
    def _():
        dk_s[...] = jnp.zeros_like(dk_s)
        dv_s[...] = jnp.zeros_like(dv_s)
        for h in range(heads):
            for j in range(seq // BLK):
                c = slice(j * BLK, (j + 1) * BLK)
                k_s[h, c, :] = qkv_ref[(3 * h + 1) * hd:(3 * h + 2) * hd, c].T
                v_s[h, c, :] = qkv_ref[(3 * h + 2) * hd:(3 * h + 3) * hd, c].T

    lo = lo_ref[i]
    cols = pl.ds(pl.multiple_of(i * BLK, BLK), BLK)
    first_row = first_ref[0:1, cols]
    delta = []
    for h in range(heads):
        hs = slice(h * hd, (h + 1) * hd)
        delta.append(jnp.sum(do_ref[hs, :].astype(jnp.float32) * o_ref[hs, :].astype(jnp.float32), axis=0, keepdims=True))
        dq_s[h] = jnp.zeros((hd, BLK), jnp.float32)

    def step(j, c):
        rows = pl.ds(pl.multiple_of(j * BLK, BLK), BLK)
        mask = visible(j, i, first_row)
        for h in range(heads):
            q_t = qkv_ref[3 * h * hd:(3 * h + 1) * hd, cols]
            do_t = do_ref[h * hd:(h + 1) * hd, :]
            s = dot32(k_s[h, rows, :], q_t) * scale
            p = jnp.exp(jnp.where(mask, s, -1e30) - lse_ref[h:h + 1, :])
            dp = dot32(v_s[h, rows, :], do_t)
            ds = (p * (dp - delta[h]) * scale).astype(jnp.bfloat16)
            pb = p.astype(jnp.bfloat16)
            dq_s[h] += dot32(qkv_ref[(3 * h + 1) * hd:(3 * h + 2) * hd, rows], ds)
            dk_s[h, :, rows] += lax.dot_general(q_t, ds, NT, preferred_element_type=jnp.float32)
            dv_s[h, :, rows] += lax.dot_general(do_t, pb, NT, preferred_element_type=jnp.float32)
        return c

    lax.fori_loop(lo, i + 1, step, 0)
    for h in range(heads):
        d_ref[3 * h * hd:(3 * h + 1) * hd, cols] = dq_s[h].astype(jnp.bfloat16)

    @pl.when(i == pl.num_programs(0) - 1)
    def _():
        for h in range(heads):
            d_ref[(3 * h + 1) * hd:(3 * h + 2) * hd, :] = dk_s[h].astype(jnp.bfloat16)
            d_ref[(3 * h + 2) * hd:(3 * h + 3) * hd, :] = dv_s[h].astype(jnp.bfloat16)


def attention_bwd(qkv_t, o_t, do_t, lse, lo, first, heads, hd):
    seq = qkv_t.shape[1]
    nb = seq // BLK
    flops = 10 * heads * seq * seq * hd // 2
    blk = lambda rows: pl.BlockSpec((rows, BLK), lambda i, lo: (0, i))
    return pl.pallas_call(
        functools.partial(attn_bwd_kernel, heads, hd),
        grid_spec=pltpu.PrefetchScalarGridSpec(
            num_scalar_prefetch=1, grid=(nb,),
            in_specs=[pl.BlockSpec(qkv_t.shape, lambda i, lo: (0, 0)), blk(heads * hd), blk(heads * hd), blk(8),
                      pl.BlockSpec((1, seq), lambda i, lo: (0, 0))],
            out_specs=pl.BlockSpec(qkv_t.shape, lambda i, lo: (0, 0)),
            scratch_shapes=[pltpu.VMEM((heads, seq, hd), jnp.bfloat16),
                            pltpu.VMEM((heads, seq, hd), jnp.bfloat16),
                            pltpu.VMEM((heads, hd, BLK), jnp.float32),
                            pltpu.VMEM((heads, hd, seq), jnp.float32),
                            pltpu.VMEM((heads, hd, seq), jnp.float32)]),
        out_shape=jax.ShapeDtypeStruct(qkv_t.shape, jnp.bfloat16),
        compiler_params=pltpu.CompilerParams(vmem_limit_bytes=56 * 2 ** 20),
        cost_estimate=pl.CostEstimate(flops=8 * flops, bytes_accessed=4 * qkv_t.size, transcendentals=0),
        name="attn_bwd",
    )(lo, qkv_t, o_t, do_t, lse, first)


def dot_nt(a, b):
    return lax.dot_general(a, b, NT, preferred_element_type=jnp.float32)


class Ring:
    def __init__(self, n):
        self.n = n
        self.me = lax.axis_index('model')
        self.core = lax.rem(self.me, 2)
        self.chip = self.me // 2
        self.partner = self.me + 1 - 2 * self.core
        self.next = lax.rem(self.me + 2, n)
        self.prev = lax.rem(self.me + n - 2, n)
        self.opp = lax.rem(self.me + n // 2, n)

    def barrier(self):
        sem = pltpu.get_barrier_semaphore()
        for dev in (self.partner, self.next, self.prev):
            pl.semaphore_signal(sem, inc=1, device_id={'model': dev}, device_id_type=MESH)
        pl.semaphore_wait(sem, 3)

    def ahead(self, d):
        return lax.rem(self.chip + d, self.n // 2)


def rows_at(start, size, unit=None):
    return pl.ds(pl.multiple_of(start, unit or size), size)


class Gather:
    def __init__(self, ring, buf, send, recv):
        self.ring, self.buf, self.send, self.recv = ring, buf, send, recv
        self.rows = buf.shape[0] // ring.n
        self.half = self.rows // 2
        r = ring
        self.table = {0: (r.me, None, r.partner),
                      1: (r.me, 0, r.next), 2: (r.me, 1, r.next), 3: (r.prev, 0, r.next),
                      4: (r.me, 1, r.prev), 5: (r.me, 0, r.prev), 6: (r.next, 1, r.prev),
                      7: (r.prev, 0, r.partner), 8: (r.prev, 1, r.partner),
                      9: (r.next, 1, r.partner), 10: (r.next, 0, r.partner),
                      11: (r.opp, 0, r.partner), 12: (r.opp, 1, r.partner)}

    def copy(self, k):
        owner, part, dev = self.table[k]
        if part is None:
            ref = self.buf.at[rows_at(owner * self.rows, self.rows)]
        else:
            ref = self.buf.at[rows_at(owner * self.rows + part * self.half, self.half)]
        return pltpu.make_async_remote_copy(src_ref=ref, dst_ref=ref, send_sem=self.send.at[k], recv_sem=self.recv.at[k],
                                            device_id={'model': dev}, device_id_type=MESH)

    def start(self, *ks):
        for k in ks:
            self.copy(k).start()

    def arrived(self, *ks):
        for k in ks:
            self.copy(k).wait_recv()

    def run(self, compute):
        self.start(1, 4, 0, 2, 5)
        self.arrived(0)
        compute(self.ring.chip)
        self.arrived(1)
        self.start(3, 7)
        self.arrived(4)
        self.start(6, 9)
        self.arrived(2)
        self.start(8)
        self.arrived(5)
        self.start(10)
        self.arrived(7, 8)
        compute(self.ring.ahead(self.ring.n // 2 - 1))
        self.arrived(9, 10)
        compute(self.ring.ahead(1))
        self.arrived(3)
        self.start(11)
        self.arrived(6)
        self.start(12)
        self.arrived(11, 12)
        compute(self.ring.ahead(self.ring.n // 4))
        for k in self.table:
            self.copy(k).wait_send()


def gather_t_kernel(n, tile, x_ref, w_ref, full_ref, out_ref, buf, w_s, stage, send, recv, load, store, put):
    ring = Ring(n)
    rows = x_ref.shape[0]
    mine = pltpu.make_async_copy(x_ref, buf.at[rows_at(ring.me * rows, rows)], load.at[0])
    mine.start()
    weights = pltpu.make_async_copy(w_ref, w_s, load.at[1])
    weights.start()
    ring.barrier()
    mine.wait()
    g = Gather(ring, buf, send, recv)
    pending = []

    def compute(chip):
        s = len(pending)
        if s == 0:
            weights.wait()
        at = rows_at(chip * (2 * rows), 2 * rows)
        keep = pltpu.make_async_copy(buf.at[at], full_ref.at[at], store.at[s])
        keep.start()

        def body(t, c):
            w_rows = rows_at(t * tile, tile)
            stage[s, w_rows, :] = dot_nt(w_s[w_rows, :], buf[at, :]).astype(jnp.bfloat16)
            return c

        lax.fori_loop(0, w_s.shape[0] // tile, body, 0)
        out = pltpu.make_async_copy(stage.at[s], out_ref.at[:, at], put.at[s])
        out.start()
        pending.append((keep, out))

    g.run(compute)
    for pair in pending:
        for cp in pair:
            cp.wait()


def gather_t(n, cid, x, w, tile):
    rows, hidden = x.shape
    seq, m, chips = rows * n, w.shape[0], n // 2
    dma = pltpu.SemaphoreType.DMA
    return pl.pallas_call(
        functools.partial(gather_t_kernel, n, tile),
        in_specs=[pl.BlockSpec(memory_space=pl.ANY)] * 2,
        out_specs=[pl.BlockSpec(memory_space=pl.ANY)] * 2,
        out_shape=[jax.ShapeDtypeStruct((seq, hidden), x.dtype), jax.ShapeDtypeStruct((m, seq), x.dtype)],
        scratch_shapes=[pltpu.VMEM((seq, hidden), x.dtype), pltpu.VMEM(w.shape, w.dtype),
                        pltpu.VMEM((chips, m, 2 * rows), x.dtype),
                        dma((13,)), dma((13,)), dma((2,)), dma((chips,)), dma((chips,))],
        compiler_params=pltpu.CompilerParams(collective_id=cid, has_side_effects=True, vmem_limit_bytes=60 * 2 ** 20),
        cost_estimate=pl.CostEstimate(flops=40 * 10 ** 9, bytes_accessed=3 * seq * hidden, transcendentals=0),
        name="gather_t",
    )(x, w)


def mlp_kernel(n, tile, x_ref, dy_ref, up_ref, down_ref, full_ref, g_ref, dz_ref,
               buf, dy_s, up_s, down_s, g_s, dz_s, send, recv, load, store, put, put2, dy_sem):
    ring = Ring(n)
    rows = x_ref.shape[0]
    mine = pltpu.make_async_copy(x_ref, buf.at[rows_at(ring.me * rows, rows)], load.at[0])
    mine.start()
    w_up = pltpu.make_async_copy(up_ref, up_s, load.at[1])
    w_up.start()
    w_down = pltpu.make_async_copy(down_ref, down_s, load.at[2])
    w_down.start()
    order = [ring.chip, ring.ahead(n // 2 - 1), ring.ahead(1), ring.ahead(n // 4)]

    def dy_copy(s):
        return pltpu.make_async_copy(dy_ref.at[rows_at(order[s] * (2 * rows), 2 * rows)], dy_s.at[s % 2], dy_sem.at[s])

    dy_copy(0).start()
    dy_copy(1).start()
    ring.barrier()
    mine.wait()
    g = Gather(ring, buf, send, recv)
    pending = []
    root = (2.0 / jnp.pi) ** 0.5

    def compute(chip):
        s = len(pending)
        if s == 0:
            w_up.wait()
            w_down.wait()
        at = rows_at(chip * (2 * rows), 2 * rows)
        keep = pltpu.make_async_copy(buf.at[at], full_ref.at[at], store.at[s])
        keep.start()
        dy_copy(s).wait()
        if s >= 2:
            for cp in pending[s - 2][1:]:
                cp.wait()

        def body(t, c):
            cols = rows_at(t * tile, tile)
            z = dot32(buf[at, :], up_s[:, cols])
            da = dot_nt(dy_s[s % 2], down_s[cols, :])
            z2 = z * z
            th = jnp.tanh(root * (z + 0.044715 * (z2 * z)))
            cdf = 0.5 * (1.0 + th)
            g_s[s % 2, :, cols] = (z * cdf).astype(jnp.bfloat16)
            slope = cdf + (0.5 * z) * (1.0 - th * th) * (root * (1.0 + (3 * 0.044715) * z2))
            dz_s[s % 2, :, cols] = (slope * da).astype(jnp.bfloat16)
            return c

        lax.fori_loop(0, up_s.shape[1] // tile, body, 0)
        if s + 2 < n // 2:
            dy_copy(s + 2).start()
        og = pltpu.make_async_copy(g_s.at[s % 2], g_ref.at[at], put.at[s])
        od = pltpu.make_async_copy(dz_s.at[s % 2], dz_ref.at[at], put2.at[s])
        og.start()
        od.start()
        pending.append((keep, og, od))

    g.run(compute)
    for s, cps in enumerate(pending):
        for cp in (cps if s >= n // 2 - 2 else cps[:1]):
            cp.wait()


def mlp(n, cid, x, dy, up, down, tile=256):
    rows, hidden = x.shape
    seq, ffn, chips = rows * n, up.shape[1], n // 2
    dma = pltpu.SemaphoreType.DMA
    return pl.pallas_call(
        functools.partial(mlp_kernel, n, tile),
        in_specs=[pl.BlockSpec(memory_space=pl.ANY)] * 4,
        out_specs=[pl.BlockSpec(memory_space=pl.ANY)] * 3,
        out_shape=[jax.ShapeDtypeStruct((seq, hidden), x.dtype)] + [jax.ShapeDtypeStruct((seq, ffn), x.dtype)] * 2,
        scratch_shapes=[pltpu.VMEM((seq, hidden), x.dtype), pltpu.VMEM((2, 2 * rows, hidden), x.dtype),
                        pltpu.VMEM(up.shape, x.dtype), pltpu.VMEM(down.shape, x.dtype),
                        pltpu.VMEM((2, 2 * rows, ffn), x.dtype), pltpu.VMEM((2, 2 * rows, ffn), x.dtype),
                        dma((13,)), dma((13,)), dma((3,)), dma((chips,)), dma((chips,)), dma((chips,)), dma((chips,))],
        compiler_params=pltpu.CompilerParams(collective_id=cid, has_side_effects=True, vmem_limit_bytes=60 * 2 ** 20),
        cost_estimate=pl.CostEstimate(flops=40 * 10 ** 9, bytes_accessed=3 * seq * hidden, transcendentals=0),
        name="gather_mlp",
    )(x, dy, up, down)


def add_rows(dst, start, count, *terms):
    step = 32

    def body(i, c):
        at = rows_at(start + i * step, step)
        total = dst[at, :].astype(jnp.float32)
        for ref, first in terms:
            total = total + ref[rows_at(first + i * step, step), :].astype(jnp.float32)
        dst[at, :] = total.astype(jnp.bfloat16)
        return c

    lax.fori_loop(0, count // step, body, 0)


class Scatter:
    def __init__(self, ring, part, pin, mid, fin, send, recv):
        self.ring, self.part, self.pin, self.mid, self.fin, self.send, self.recv = ring, part, pin, mid, fin, send, recv
        self.rows = part.shape[1] // 2
        self.half = self.rows // 2
        self.own = ring.core * self.rows

    def copy(self, k):
        r, h = self.ring, self.half
        if k < 4:
            src, dst, dev = self.part.at[k, rows_at((1 - r.core) * self.rows, self.rows)], self.pin.at[k], r.partner
        else:
            d, half, dst, dev = {4: (2, 0, self.mid.at[0], r.next), 5: (2, 1, self.mid.at[1], r.prev),
                                 6: (1, 1, self.fin.at[0, h:], r.next), 7: (1, 0, self.fin.at[0, :h], r.next),
                                 8: (3, 0, self.fin.at[1, :h], r.prev), 9: (3, 1, self.fin.at[1, h:], r.prev)}[k]
            src = self.part.at[d, rows_at(self.own + half * h, h)]
        return pltpu.make_async_remote_copy(src_ref=src, dst_ref=dst, send_sem=self.send.at[k], recv_sem=self.recv.at[k],
                                            device_id={'model': dev}, device_id_type=MESH)

    def start(self, k):
        self.copy(k).start()

    def arrived(self, k):
        self.copy(k).wait_recv()

    def join(self, d):
        self.arrived(d)
        add_rows(self.part.at[d], self.own, self.rows, (self.pin.at[d], 0))

    def run(self, product, filler, out_ref):
        h = self.half
        product(2)
        self.start(2)
        product(1)
        self.start(1)
        self.join(2)
        self.start(4)
        self.start(5)
        product(3)
        self.start(3)
        self.join(1)
        self.start(6)
        self.join(3)
        self.start(8)
        product(0)
        self.start(0)
        self.join(0)
        self.arrived(4)
        add_rows(self.part.at[1], self.own, h, (self.mid.at[0], 0))
        self.start(7)
        self.arrived(5)
        add_rows(self.part.at[3], self.own + h, h, (self.mid.at[1], 0))
        self.start(9)
        filler()
        for k in (6, 7, 8, 9):
            self.arrived(k)
        step = 32

        def body(i, c):
            at = rows_at(i * step, step)
            total = self.part[0, rows_at(self.own + i * step, step), :].astype(jnp.float32)
            total = total + self.fin[0, at, :].astype(jnp.float32) + self.fin[1, at, :].astype(jnp.float32)
            out_ref[at, :] = total.astype(jnp.bfloat16)
            return c

        lax.fori_loop(0, self.rows // step, body, 0)
        for k in range(10):
            self.copy(k).wait_send()


def scatter_scratch(rows, hidden, dtype):
    dma = pltpu.SemaphoreType.DMA
    return [pltpu.VMEM((4, 2 * rows, hidden), dtype), pltpu.VMEM((4, rows, hidden), dtype),
            pltpu.VMEM((2, rows // 2, hidden), dtype), pltpu.VMEM((2, rows, hidden), dtype), dma((10,)), dma((10,))]


def scatter_t_kernel(n, tile, x_ref, w_ref, out_ref, x_s, w_s, lhs, part, pin, mid, fin, send, recv, load):
    ring = Ring(n)
    cx = pltpu.make_async_copy(x_ref, x_s, load.at[0])
    cx.start()
    cw = pltpu.make_async_copy(w_ref, w_s, load.at[1])
    cw.start()
    ring.barrier()
    cx.wait()
    cw.wait()
    sc = Scatter(ring, part, pin, mid, fin, send, recv)
    wide = part.shape[1]

    def product(d):
        at = rows_at(ring.ahead(d) * wide, wide)
        lhs[...] = x_s[:, at].T

        def body(t, c):
            cols = rows_at(t * tile, tile)
            part[d, :, cols] = dot32(lhs[...], w_s[:, cols]).astype(jnp.bfloat16)
            return c

        lax.fori_loop(0, w_s.shape[1] // tile, body, 0)

    sc.run(product, lambda: None, out_ref)


def scatter_t(n, cid, x, w, tile=512):
    (m, seq), hidden = x.shape, w.shape[1]
    rows = seq // n
    dma = pltpu.SemaphoreType.DMA
    return pl.pallas_call(
        functools.partial(scatter_t_kernel, n, tile),
        in_specs=[pl.BlockSpec(memory_space=pl.ANY)] * 2,
        out_specs=pl.BlockSpec(memory_space=pltpu.VMEM),
        out_shape=jax.ShapeDtypeStruct((rows, hidden), x.dtype),
        scratch_shapes=[pltpu.VMEM(x.shape, x.dtype), pltpu.VMEM(w.shape, x.dtype), pltpu.VMEM((2 * rows, m), x.dtype)]
        + scatter_scratch(rows, hidden, x.dtype) + [dma((2,))],
        compiler_params=pltpu.CompilerParams(collective_id=cid, has_side_effects=True, vmem_limit_bytes=60 * 2 ** 20),
        cost_estimate=pl.CostEstimate(flops=40 * 10 ** 9, bytes_accessed=3 * seq * hidden, transcendentals=0),
        name="scatter_t",
    )(x, w)


def scatter_mlp_kernel(n, tile, dz_ref, up_ref, g_ref, down_ref, out_ref, y_ref,
                       dz_s, w_s, g_s, down_s, part, pin, mid, fin, send, recv, load, ystage, put):
    ring = Ring(n)
    loads = [pltpu.make_async_copy(a, b, load.at[i]) for i, (a, b) in
             enumerate(((dz_ref, dz_s), (up_ref, w_s), (g_ref, g_s), (down_ref, down_s)))]
    for cp in loads:
        cp.start()
    ring.barrier()
    loads[0].wait()
    loads[1].wait()
    sc = Scatter(ring, part, pin, mid, fin, send, recv)
    wide = part.shape[1]
    hidden = part.shape[2]

    def product(d):
        at = rows_at(ring.ahead(d) * wide, wide)

        def body(t, c):
            cols = rows_at(t * tile, tile)
            part[d, :, cols] = dot_nt(dz_s[at, :], w_s[cols, :]).astype(jnp.bfloat16)
            return c

        lax.fori_loop(0, hidden // tile, body, 0)

    def filler():
        loads[2].wait()
        loads[3].wait()
        puts = []
        for q in range(n // 2):
            if q >= 2:
                puts[q - 2].wait()

            def body(t, c):
                cols = rows_at(t * tile, tile)
                ystage[q % 2, :, cols] = dot32(g_s[q * wide:(q + 1) * wide, :], down_s[:, cols]).astype(jnp.bfloat16)
                return c

            lax.fori_loop(0, hidden // tile, body, 0)
            puts.append(pltpu.make_async_copy(ystage.at[q % 2], y_ref.at[q * wide:(q + 1) * wide], put.at[q]))
            puts[q].start()
        for cp in puts[-2:]:
            cp.wait()

    sc.run(product, filler, out_ref)


def scatter_mlp(n, cid, dz, up, g, down, tile=512):
    (seq, ffn), hidden = dz.shape, down.shape[1]
    rows = seq // n
    dma = pltpu.SemaphoreType.DMA
    return pl.pallas_call(
        functools.partial(scatter_mlp_kernel, n, tile),
        in_specs=[pl.BlockSpec(memory_space=pl.ANY)] * 4,
        out_specs=[pl.BlockSpec(memory_space=pltpu.VMEM), pl.BlockSpec(memory_space=pl.ANY)],
        out_shape=[jax.ShapeDtypeStruct((rows, hidden), dz.dtype), jax.ShapeDtypeStruct((seq, hidden), dz.dtype)],
        scratch_shapes=[pltpu.VMEM(a.shape, a.dtype) for a in (dz, up, g, down)]
        + scatter_scratch(rows, hidden, dz.dtype) + [dma((4,)), pltpu.VMEM((2, 2 * rows, hidden), dz.dtype), dma((n // 2,))],
        compiler_params=pltpu.CompilerParams(collective_id=cid, has_side_effects=True, vmem_limit_bytes=63 * 2 ** 20),
        cost_estimate=pl.CostEstimate(flops=60 * 10 ** 9, bytes_accessed=3 * seq * hidden, transcendentals=0),
        name="scatter_mlp",
    )(dz, up, g, down)


def group_sum(vals, n):
    total = vals
    for shift in range(1, n):
        total = total + lax.ppermute(vals, 'model', [(a, (a + shift) % n) for a in range(n)])
    return total


def local_layer(n, hidden_in, seg_ids, gain_attn, w_qkv, w_out, gain_mlp, w_up, w_down, grad_out):
    heads, hd, hidden = w_out.shape
    seq_len = seg_ids.shape[1]
    x_f32 = hidden_in[0].astype(jnp.float32)
    dy = grad_out[0]
    wq_t = jnp.transpose(w_qkv, (1, 2, 3, 0)).reshape(heads * 3 * hd, hidden)
    wo = w_out.reshape(heads * hd, hidden)
    first = jnp.sum(seg_ids[0][:, None] < seg_ids[0][None, :], axis=0, dtype=jnp.int32)
    lo = first[::BLK] // BLK
    first = first[None]
    ein = functools.partial(jnp.einsum, preferred_element_type=jnp.float32)
    gather = lambda a: lax.all_gather(a, 'model', axis=0, tiled=True)
    scatter = lambda a: lax.psum_scatter(a, 'model', scatter_dimension=0, tiled=True)

    ln1_out, ln1_vjp = jax.vjp(layer_norm, x_f32, gain_attn.astype(jnp.float32))
    attn_in, qkv_t = gather_t(n, 0, ln1_out.astype(jnp.bfloat16), wq_t, 320)
    dy_late, qkv_t = lax.optimization_barrier((dy, qkv_t))
    grad_full = gather(dy_late)
    o_t, lse = attention_fwd(qkv_t, lo, first, heads, hd)
    attn_sum = scatter_t(n, 1, o_t, wo)
    mid_loc = (x_f32 + attn_sum.astype(jnp.float32)).astype(jnp.bfloat16)
    ln2_out, ln2_vjp = jax.vjp(layer_norm, mid_loc.astype(jnp.float32), gain_mlp.astype(jnp.float32))
    mlp_in, act_lo, d_pre = mlp(n, 2, ln2_out.astype(jnp.bfloat16), grad_full, w_up, w_down)
    d_mlp_in, mlp_part = scatter_mlp(n, 3, d_pre, w_up, act_lo, w_down)
    d_mid_ln, d_gain_mlp = ln2_vjp(d_mlp_in.astype(jnp.float32))
    d_mid = (dy.astype(jnp.float32) + d_mid_ln).astype(jnp.bfloat16)
    d_mid_full, do_t = gather_t(n, 4, d_mid, wo, heads * hd)
    mlp_part, do_t = lax.optimization_barrier((mlp_part, do_t))
    mlp_sum = scatter(mlp_part)
    hidden_out = (mid_loc.astype(jnp.float32) + mlp_sum.astype(jnp.float32)).astype(jnp.bfloat16)
    dqkv_t = attention_bwd(qkv_t, o_t, do_t, lse, lo, first, heads, hd)
    d_attn_in = scatter_t(n, 5, dqkv_t, wq_t)
    g_down = ein('sf,sd->fd', act_lo, grad_full).astype(jnp.bfloat16)
    g_up = ein('sd,sf->df', mlp_in, d_pre).astype(jnp.bfloat16)
    g_out = ein('es,sd->ed', o_t, d_mid_full).astype(jnp.bfloat16)
    g_qkv = ein('ns,sd->nd', dqkv_t, attn_in).astype(jnp.bfloat16)
    d_x_ln, d_gain_attn = ln1_vjp(d_attn_in.astype(jnp.float32))
    grad_in = (d_mid.astype(jnp.float32) + d_x_ln).astype(jnp.bfloat16)
    gain_sums = group_sum(jnp.stack([d_gain_attn, d_gain_mlp]), n).astype(jnp.bfloat16)
    g_qkv = jnp.transpose(g_qkv.reshape(heads, 3, hd, hidden), (3, 0, 1, 2))
    return (hidden_out[None], grad_in[None], g_qkv, g_out.reshape(heads, hd, hidden), g_up, g_down,
            gain_sums[0], gain_sums[1])


def solution(mesh):
    act_spec = P('data', 'model', None)
    in_specs = (act_spec, P('data', None), P(), P(None, 'model', None, None), P('model', None, None), P(), P(None, 'model'), P('model', None), act_spec)
    out_specs = (act_spec, act_spec, P('data', 'model', None, None), P(('data', 'model'), None, None), P('data', 'model'), P(('data', 'model'), None), P('data'), P('data'))
    return jax.shard_map(functools.partial(local_layer, mesh.shape['model']), mesh=mesh, in_specs=in_specs, out_specs=out_specs, check_vma=False)
```

```python
import functools

import jax
import jax.numpy as jnp
from jax import lax
from jax.experimental import pallas as pl
from jax.experimental.pallas import tpu as pltpu
from jax.sharding import PartitionSpec as P

LN_EPS = 1e-5
BLK = 256
NT = (((1,), (1,)), ((), ()))
MESH = pl.DeviceIdType.MESH


def layer_norm(x_f32, gain_f32):
    mean_val = jnp.mean(x_f32, axis=-1, keepdims=True)
    centered = x_f32 - mean_val
    variance = jnp.mean(centered * centered, axis=-1, keepdims=True)
    return centered * lax.rsqrt(variance + LN_EPS) * gain_f32


def gelu_tanh(pre_act):
    return jax.nn.gelu(pre_act, approximate=True)


def dot32(a, b):
    return jnp.dot(a, b, preferred_element_type=jnp.float32)


def visible(j, i, first_row):
    kpos = j * BLK + lax.broadcasted_iota(jnp.int32, (BLK, BLK), 0)
    qpos = i * BLK + lax.broadcasted_iota(jnp.int32, (BLK, BLK), 1)
    return (kpos <= qpos) & (kpos >= first_row)


def attn_fwd_kernel(heads, hd, lo_ref, qkv_ref, first_ref, o_ref, lse_ref, k_s, s_s, o_s):
    i = pl.program_id(0)
    scale = hd ** -0.5

    @pl.when(i == 0)
    def _():
        for h in range(heads):
            for j in range(k_s.shape[1] // BLK):
                kt = qkv_ref[(3 * h + 1) * hd:(3 * h + 2) * hd, j * BLK:(j + 1) * BLK]
                k_s[h, j * BLK:(j + 1) * BLK, :] = kt.T

    lo = lo_ref[i]
    cols = pl.ds(pl.multiple_of(i * BLK, BLK), BLK)
    first_row = first_ref[0:1, cols]
    neg = jnp.full((8, BLK), -jnp.inf, jnp.float32)

    def scores(j, m):
        rows = pl.ds(pl.multiple_of(j * BLK, BLK), BLK)
        mask = visible(j, i, first_row)
        out = []
        for h in range(heads):
            s = dot32(k_s[h, rows, :], qkv_ref[3 * h * hd:(3 * h + 1) * hd, cols]) * scale
            s = jnp.where(mask, s, -1e30)
            s_s[h, rows, :] = s
            out.append(jnp.maximum(m[h], jnp.max(s.reshape(BLK // 8, 8, BLK), axis=0)))
        return tuple(out)

    m = lax.fori_loop(lo, i + 1, scores, (neg,) * heads)
    m = [jnp.max(x, axis=0, keepdims=True) for x in m]

    def expo(j, l):
        rows = pl.ds(pl.multiple_of(j * BLK, BLK), BLK)
        out = []
        for h in range(heads):
            e = jnp.exp(s_s[h, rows, :] - m[h])
            s_s[h, rows, :] = e
            out.append(l[h] + jnp.sum(e.reshape(BLK // 8, 8, BLK), axis=0))
        return tuple(out)

    l = lax.fori_loop(lo, i + 1, expo, (jnp.zeros((8, BLK), jnp.float32),) * heads)
    l = [jnp.sum(x, axis=0, keepdims=True) for x in l]
    r = [1.0 / x for x in l]
    for h in range(heads):
        lse_ref[h:h + 1, :] = m[h] + jnp.log(l[h])
        o_s[h] = jnp.zeros((hd, BLK), jnp.float32)

    def values(j, c):
        rows = pl.ds(pl.multiple_of(j * BLK, BLK), BLK)
        for h in range(heads):
            pb = (s_s[h, rows, :] * r[h]).astype(jnp.bfloat16)
            o_s[h] += dot32(qkv_ref[(3 * h + 2) * hd:(3 * h + 3) * hd, rows], pb)
        return c

    lax.fori_loop(lo, i + 1, values, 0)
    for h in range(heads):
        o_ref[h * hd:(h + 1) * hd, :] = o_s[h].astype(jnp.bfloat16)


def attention_fwd(qkv_t, lo, first, heads, hd):
    seq = qkv_t.shape[1]
    nb = seq // BLK
    flops = 4 * heads * seq * seq * hd // 2
    return pl.pallas_call(
        functools.partial(attn_fwd_kernel, heads, hd),
        grid_spec=pltpu.PrefetchScalarGridSpec(
            num_scalar_prefetch=1, grid=(nb,),
            in_specs=[pl.BlockSpec(qkv_t.shape, lambda i, lo: (0, 0)),
                      pl.BlockSpec((1, seq), lambda i, lo: (0, 0))],
            out_specs=[pl.BlockSpec((heads * hd, BLK), lambda i, lo: (0, i)),
                       pl.BlockSpec((8, BLK), lambda i, lo: (0, i))],
            scratch_shapes=[pltpu.VMEM((heads, seq, hd), jnp.bfloat16),
                            pltpu.VMEM((heads, seq, BLK), jnp.float32),
                            pltpu.VMEM((heads, hd, BLK), jnp.float32)]),
        out_shape=[jax.ShapeDtypeStruct((heads * hd, seq), jnp.bfloat16),
                   jax.ShapeDtypeStruct((8, seq), jnp.float32)],
        compiler_params=pltpu.CompilerParams(vmem_limit_bytes=56 * 2 ** 20),
        cost_estimate=pl.CostEstimate(flops=8 * flops, bytes_accessed=2 * qkv_t.size, transcendentals=0),
        name="attn_fwd",
    )(lo, qkv_t, first)


def attn_bwd_kernel(heads, hd, lo_ref, qkv_ref, o_ref, do_ref, lse_ref, first_ref, d_ref,
                    k_s, v_s, dq_s, dk_s, dv_s):
    i = pl.program_id(0)
    seq = qkv_ref.shape[1]
    scale = hd ** -0.5

    @pl.when(i == 0)
    def _():
        dk_s[...] = jnp.zeros_like(dk_s)
        dv_s[...] = jnp.zeros_like(dv_s)
        for h in range(heads):
            for j in range(seq // BLK):
                c = slice(j * BLK, (j + 1) * BLK)
                k_s[h, c, :] = qkv_ref[(3 * h + 1) * hd:(3 * h + 2) * hd, c].T
                v_s[h, c, :] = qkv_ref[(3 * h + 2) * hd:(3 * h + 3) * hd, c].T

    lo = lo_ref[i]
    cols = pl.ds(pl.multiple_of(i * BLK, BLK), BLK)
    first_row = first_ref[0:1, cols]
    delta = []
    for h in range(heads):
        hs = slice(h * hd, (h + 1) * hd)
        delta.append(jnp.sum(do_ref[hs, :].astype(jnp.float32) * o_ref[hs, :].astype(jnp.float32), axis=0, keepdims=True))
        dq_s[h] = jnp.zeros((hd, BLK), jnp.float32)

    def step(j, c):
        rows = pl.ds(pl.multiple_of(j * BLK, BLK), BLK)
        mask = visible(j, i, first_row)
        for h in range(heads):
            q_t = qkv_ref[3 * h * hd:(3 * h + 1) * hd, cols]
            do_t = do_ref[h * hd:(h + 1) * hd, :]
            s = dot32(k_s[h, rows, :], q_t) * scale
            p = jnp.exp(jnp.where(mask, s, -1e30) - lse_ref[h:h + 1, :])
            dp = dot32(v_s[h, rows, :], do_t)
            ds = (p * (dp - delta[h]) * scale).astype(jnp.bfloat16)
            pb = p.astype(jnp.bfloat16)
            dq_s[h] += dot32(qkv_ref[(3 * h + 1) * hd:(3 * h + 2) * hd, rows], ds)
            dk_s[h, :, rows] += lax.dot_general(q_t, ds, NT, preferred_element_type=jnp.float32)
            dv_s[h, :, rows] += lax.dot_general(do_t, pb, NT, preferred_element_type=jnp.float32)
        return c

    lax.fori_loop(lo, i + 1, step, 0)
    for h in range(heads):
        d_ref[3 * h * hd:(3 * h + 1) * hd, cols] = dq_s[h].astype(jnp.bfloat16)

    @pl.when(i == pl.num_programs(0) - 1)
    def _():
        for h in range(heads):
            d_ref[(3 * h + 1) * hd:(3 * h + 2) * hd, :] = dk_s[h].astype(jnp.bfloat16)
            d_ref[(3 * h + 2) * hd:(3 * h + 3) * hd, :] = dv_s[h].astype(jnp.bfloat16)


def attention_bwd(qkv_t, o_t, do_t, lse, lo, first, heads, hd):
    seq = qkv_t.shape[1]
    nb = seq // BLK
    flops = 10 * heads * seq * seq * hd // 2
    blk = lambda rows: pl.BlockSpec((rows, BLK), lambda i, lo: (0, i))
    return pl.pallas_call(
        functools.partial(attn_bwd_kernel, heads, hd),
        grid_spec=pltpu.PrefetchScalarGridSpec(
            num_scalar_prefetch=1, grid=(nb,),
            in_specs=[pl.BlockSpec(qkv_t.shape, lambda i, lo: (0, 0)), blk(heads * hd), blk(heads * hd), blk(8),
                      pl.BlockSpec((1, seq), lambda i, lo: (0, 0))],
            out_specs=pl.BlockSpec(qkv_t.shape, lambda i, lo: (0, 0)),
            scratch_shapes=[pltpu.VMEM((heads, seq, hd), jnp.bfloat16),
                            pltpu.VMEM((heads, seq, hd), jnp.bfloat16),
                            pltpu.VMEM((heads, hd, BLK), jnp.float32),
                            pltpu.VMEM((heads, hd, seq), jnp.float32),
                            pltpu.VMEM((heads, hd, seq), jnp.float32)]),
        out_shape=jax.ShapeDtypeStruct(qkv_t.shape, jnp.bfloat16),
        compiler_params=pltpu.CompilerParams(vmem_limit_bytes=56 * 2 ** 20),
        cost_estimate=pl.CostEstimate(flops=8 * flops, bytes_accessed=4 * qkv_t.size, transcendentals=0),
        name="attn_bwd",
    )(lo, qkv_t, o_t, do_t, lse, first)


def dot_nt(a, b):
    return lax.dot_general(a, b, NT, preferred_element_type=jnp.float32)


class Ring:
    def __init__(self, n):
        self.n = n
        self.me = lax.axis_index('model')
        self.core = lax.rem(self.me, 2)
        self.chip = self.me // 2
        self.partner = self.me + 1 - 2 * self.core
        self.next = lax.rem(self.me + 2, n)
        self.prev = lax.rem(self.me + n - 2, n)
        self.opp = lax.rem(self.me + n // 2, n)

    def barrier(self):
        sem = pltpu.get_barrier_semaphore()
        for dev in (self.partner, self.next, self.prev):
            pl.semaphore_signal(sem, inc=1, device_id={'model': dev}, device_id_type=MESH)
        pl.semaphore_wait(sem, 3)

    def ahead(self, d):
        return lax.rem(self.chip + d, self.n // 2)


def rows_at(start, size, unit=None):
    return pl.ds(pl.multiple_of(start, unit or size), size)


class Gather:
    def __init__(self, ring, buf, send, recv):
        self.ring, self.buf, self.send, self.recv = ring, buf, send, recv
        self.rows = buf.shape[0] // ring.n
        self.half = self.rows // 2
        r = ring
        self.table = {0: (r.me, None, r.partner),
                      1: (r.me, 0, r.next), 2: (r.me, 1, r.next), 3: (r.prev, 0, r.next),
                      4: (r.me, 1, r.prev), 5: (r.me, 0, r.prev), 6: (r.next, 1, r.prev),
                      7: (r.prev, 0, r.partner), 8: (r.prev, 1, r.partner),
                      9: (r.next, 1, r.partner), 10: (r.next, 0, r.partner),
                      11: (r.opp, 0, r.partner), 12: (r.opp, 1, r.partner)}

    def copy(self, k):
        owner, part, dev = self.table[k]
        if part is None:
            ref = self.buf.at[rows_at(owner * self.rows, self.rows)]
        else:
            ref = self.buf.at[rows_at(owner * self.rows + part * self.half, self.half)]
        return pltpu.make_async_remote_copy(src_ref=ref, dst_ref=ref, send_sem=self.send.at[k], recv_sem=self.recv.at[k],
                                            device_id={'model': dev}, device_id_type=MESH)

    def start(self, *ks):
        for k in ks:
            self.copy(k).start()

    def arrived(self, *ks):
        for k in ks:
            self.copy(k).wait_recv()

    def run(self, compute, fill=lambda k: None):
        self.start(1, 4, 0, 2, 5)
        self.arrived(0)
        compute(self.ring.chip)
        fill(0)
        self.arrived(1)
        self.start(3, 7)
        self.arrived(4)
        self.start(6, 9)
        fill(1)
        self.arrived(2)
        self.start(8)
        self.arrived(5)
        self.start(10)
        self.arrived(7, 8)
        compute(self.ring.ahead(self.ring.n // 2 - 1))
        self.arrived(9, 10)
        compute(self.ring.ahead(1))
        fill(2)
        self.arrived(3)
        self.start(11)
        self.arrived(6)
        self.start(12)
        self.arrived(11, 12)
        compute(self.ring.ahead(self.ring.n // 4))
        for k in self.table:
            self.copy(k).wait_send()


def gather_t_kernel(n, tile, x_ref, w_ref, full_ref, out_ref, buf, w_s, stage, send, recv, load, store, put):
    ring = Ring(n)
    rows = x_ref.shape[0]
    mine = pltpu.make_async_copy(x_ref, buf.at[rows_at(ring.me * rows, rows)], load.at[0])
    mine.start()
    weights = pltpu.make_async_copy(w_ref, w_s, load.at[1])
    weights.start()
    ring.barrier()
    mine.wait()
    g = Gather(ring, buf, send, recv)
    pending = []

    def compute(chip):
        s = len(pending)
        if s == 0:
            weights.wait()
        at = rows_at(chip * (2 * rows), 2 * rows)
        keep = pltpu.make_async_copy(buf.at[at], full_ref.at[at], store.at[s])
        keep.start()

        def body(t, c):
            w_rows = rows_at(t * tile, tile)
            stage[s, w_rows, :] = dot_nt(w_s[w_rows, :], buf[at, :]).astype(jnp.bfloat16)
            return c

        lax.fori_loop(0, w_s.shape[0] // tile, body, 0)
        out = pltpu.make_async_copy(stage.at[s], out_ref.at[:, at], put.at[s])
        out.start()
        pending.append((keep, out))

    g.run(compute)
    for pair in pending:
        for cp in pair:
            cp.wait()


def gather_t(n, cid, x, w, tile):
    rows, hidden = x.shape
    seq, m, chips = rows * n, w.shape[0], n // 2
    dma = pltpu.SemaphoreType.DMA
    return pl.pallas_call(
        functools.partial(gather_t_kernel, n, tile),
        in_specs=[pl.BlockSpec(memory_space=pl.ANY)] * 2,
        out_specs=[pl.BlockSpec(memory_space=pl.ANY)] * 2,
        out_shape=[jax.ShapeDtypeStruct((seq, hidden), x.dtype), jax.ShapeDtypeStruct((m, seq), x.dtype)],
        scratch_shapes=[pltpu.VMEM((seq, hidden), x.dtype), pltpu.VMEM(w.shape, w.dtype),
                        pltpu.VMEM((chips, m, 2 * rows), x.dtype),
                        dma((13,)), dma((13,)), dma((2,)), dma((chips,)), dma((chips,))],
        compiler_params=pltpu.CompilerParams(collective_id=cid, has_side_effects=True, vmem_limit_bytes=60 * 2 ** 20),
        cost_estimate=pl.CostEstimate(flops=40 * 10 ** 9, bytes_accessed=3 * seq * hidden, transcendentals=0),
        name="gather_t",
    )(x, w)


def mlp_kernel(n, tile, x_ref, dy_ref, up_ref, down_ref, full_ref, g_ref, dz_ref,
               buf, dy_s, up_s, down_s, g_s, dz_s, da_s, send, recv, load, store, put, put2, dy_sem):
    ring = Ring(n)
    rows = x_ref.shape[0]
    mine = pltpu.make_async_copy(x_ref, buf.at[rows_at(ring.me * rows, rows)], load.at[0])
    mine.start()
    w_up = pltpu.make_async_copy(up_ref, up_s, load.at[1])
    w_up.start()
    w_down = pltpu.make_async_copy(down_ref, down_s, load.at[2])
    w_down.start()
    order = [ring.chip, ring.ahead(n // 2 - 1), ring.ahead(1), ring.ahead(n // 4)]

    def dy_copy(s):
        return pltpu.make_async_copy(dy_ref.at[rows_at(order[s] * (2 * rows), 2 * rows)], dy_s.at[s % 2], dy_sem.at[s])

    dy_copy(0).start()
    dy_copy(1).start()
    ring.barrier()
    mine.wait()
    g = Gather(ring, buf, send, recv)
    pending = []
    root = (2.0 / jnp.pi) ** 0.5

    def compute(chip):
        s = len(pending)
        if s == 0:
            w_up.wait()
            w_down.wait()
        at = rows_at(chip * (2 * rows), 2 * rows)
        keep = pltpu.make_async_copy(buf.at[at], full_ref.at[at], store.at[s])
        keep.start()
        if s >= 2:
            for cp in pending[s - 2][1:]:
                cp.wait()
        if s == 0:
            dy_copy(0).wait()

        def body(t, c):
            cols = rows_at(t * tile, tile)
            z = dot32(buf[at, :], up_s[:, cols])
            if s == 0:
                da = dot_nt(dy_s[0], down_s[cols, :])
            else:
                da = da_s[s - 1, :, cols]
            z2 = z * z
            th = jnp.tanh(root * (z + 0.044715 * (z2 * z)))
            cdf = 0.5 * (1.0 + th)
            g_s[s % 2, :, cols] = (z * cdf).astype(jnp.bfloat16)
            slope = cdf + (0.5 * z) * (1.0 - th * th) * (root * (1.0 + (3 * 0.044715) * z2))
            dz_s[s % 2, :, cols] = (slope * da).astype(jnp.bfloat16)
            return c

        lax.fori_loop(0, up_s.shape[1] // tile, body, 0)
        if s == 0:
            dy_copy(2).start()
        og = pltpu.make_async_copy(g_s.at[s % 2], g_ref.at[at], put.at[s])
        od = pltpu.make_async_copy(dz_s.at[s % 2], dz_ref.at[at], put2.at[s])
        og.start()
        od.start()
        pending.append((keep, og, od))

    def fill(k):
        if k == 1:
            for s in range(1, n // 2):
                dy_copy(s).wait()

                def body(t, c):
                    cols = rows_at(t * tile, tile)
                    da_s[s - 1, :, cols] = dot_nt(dy_s[s % 2], down_s[cols, :])
                    return c

                lax.fori_loop(0, up_s.shape[1] // tile, body, 0)
                if s + 2 < n // 2:
                    dy_copy(s + 2).start()

    g.run(compute, fill)
    for s, cps in enumerate(pending):
        for cp in (cps if s >= n // 2 - 2 else cps[:1]):
            cp.wait()


def mlp(n, cid, x, dy, up, down, tile=256):
    rows, hidden = x.shape
    seq, ffn, chips = rows * n, up.shape[1], n // 2
    dma = pltpu.SemaphoreType.DMA
    return pl.pallas_call(
        functools.partial(mlp_kernel, n, tile),
        in_specs=[pl.BlockSpec(memory_space=pl.ANY)] * 4,
        out_specs=[pl.BlockSpec(memory_space=pl.ANY)] * 3,
        out_shape=[jax.ShapeDtypeStruct((seq, hidden), x.dtype)] + [jax.ShapeDtypeStruct((seq, ffn), x.dtype)] * 2,
        scratch_shapes=[pltpu.VMEM((seq, hidden), x.dtype), pltpu.VMEM((2, 2 * rows, hidden), x.dtype),
                        pltpu.VMEM(up.shape, x.dtype), pltpu.VMEM(down.shape, x.dtype),
                        pltpu.VMEM((2, 2 * rows, ffn), x.dtype), pltpu.VMEM((2, 2 * rows, ffn), x.dtype),
                        pltpu.VMEM((chips - 1, 2 * rows, ffn), jnp.float32),
                        dma((13,)), dma((13,)), dma((3,)), dma((chips,)), dma((chips,)), dma((chips,)), dma((chips,))],
        compiler_params=pltpu.CompilerParams(collective_id=cid, has_side_effects=True, vmem_limit_bytes=60 * 2 ** 20),
        cost_estimate=pl.CostEstimate(flops=40 * 10 ** 9, bytes_accessed=3 * seq * hidden, transcendentals=0),
        name="gather_mlp",
    )(x, dy, up, down)


class Product:
    def __init__(self, x, fixed, out, slots, stage, load, store, rows, lhs=None):
        self.x, self.fixed, self.out, self.slots, self.stage = x, fixed, out, slots, stage
        self.load, self.store, self.rows, self.lhs = load, store, rows, lhs
        self.unit = slots.shape[2]
        self.total = x.shape[1] // self.unit

    def get(self, u):
        slot = lax.rem(u, 2)
        return pltpu.make_async_copy(self.x.at[:, rows_at(u * self.unit, self.unit)], self.slots.at[slot], self.load.at[slot])

    def put(self, u):
        slot = lax.rem(u, 2)
        at = rows_at(u * self.unit, self.unit)
        dst = self.out.at[at] if self.rows else self.out.at[:, at]
        return pltpu.make_async_copy(self.stage.at[slot], dst, self.store.at[slot])

    def run(self, first, last):
        def body(u, c):
            slot = lax.rem(u, 2)
            self.get(u).wait()

            @pl.when(u + 1 < self.total)
            def _():
                self.get(u + 1).start()

            @pl.when(u >= 2)
            def _():
                self.put(u - 2).wait()

            if self.rows:
                self.lhs[...] = self.slots[slot].T
                width = self.fixed.shape[1]
                for w in range(0, width, 1280):
                    at = slice(w, min(w + 1280, width))
                    self.stage[slot, :, at] = dot32(self.lhs[...], self.fixed[:, at]).astype(jnp.bfloat16)
            else:
                step = 320

                def part(t, c):
                    at = rows_at(t * step, step)
                    self.stage[slot, at, :] = dot32(self.fixed[at, :], self.slots[slot]).astype(jnp.bfloat16)
                    return c

                lax.fori_loop(0, self.fixed.shape[0] // step, part, 0)
            self.put(u).start()
            return c

        lax.fori_loop(first, last, body, 0)

    def finish(self):
        self.put(self.total - 2).wait()
        self.put(self.total - 1).wait()


def gather_grads_kernel(n, x_ref, w_ref, b_ref, dz_ref, g_ref, dy_ref, full_ref, out_ref, up_ref, down_ref,
                        buf, w_s, stage, dz_s, dy_s, b_s, g_s, lhs, up_st, down_st,
                        send, recv, load, store, put, up_l, up_p, down_l, down_p):
    ring = Ring(n)
    rows = x_ref.shape[0]
    loads = [pltpu.make_async_copy(a, b, load.at[i]) for i, (a, b) in
             enumerate(((x_ref, buf.at[rows_at(ring.me * rows, rows)]), (w_ref, w_s), (dz_ref, dz_s), (dy_ref, dy_s)))]
    up = Product(b_ref, dz_s, up_ref, b_s, up_st, up_l, up_p, True, lhs)
    down = Product(g_ref, dy_s, down_ref, g_s, down_st, down_l, down_p, True, lhs)
    loads[0].start()
    loads[1].start()
    up.get(0).start()
    loads[2].start()
    down.get(0).start()
    loads[3].start()
    ring.barrier()
    loads[0].wait()
    g = Gather(ring, buf, send, recv)
    pending = []

    def compute(chip):
        s = len(pending)
        if s == 0:
            loads[1].wait()
        at = rows_at(chip * (2 * rows), 2 * rows)
        keep = pltpu.make_async_copy(buf.at[at], full_ref.at[at], store.at[s])
        keep.start()
        stage[s] = dot_nt(w_s[...], buf[at, :]).astype(jnp.bfloat16)
        out = pltpu.make_async_copy(stage.at[s], out_ref.at[:, at], put.at[s])
        out.start()
        pending.append((keep, out))

    def fill(k):
        mid = up.total // 2
        if k == 0:
            loads[2].wait()
            up.run(0, mid)
        elif k == 1:
            up.run(mid, up.total)
            loads[3].wait()
            down.run(0, down.total // 2)
        else:
            down.run(down.total // 2, down.total)

    g.run(compute, fill)
    up.finish()
    down.finish()
    for pair in pending:
        for cp in pair:
            cp.wait()


def gather_grads(n, cid, x, w, b1, dz, g, dy, unit=256):
    rows, hidden = x.shape
    seq, m, chips, ffn = rows * n, w.shape[0], n // 2, dz.shape[1]
    dma = pltpu.SemaphoreType.DMA
    shape = lambda *d: jax.ShapeDtypeStruct(d, x.dtype)
    vmem = lambda *d: pltpu.VMEM(d, x.dtype)
    return pl.pallas_call(
        functools.partial(gather_grads_kernel, n),
        in_specs=[pl.BlockSpec(memory_space=pl.ANY)] * 6,
        out_specs=[pl.BlockSpec(memory_space=pl.ANY)] * 4,
        out_shape=[shape(seq, hidden), shape(m, seq), shape(hidden, ffn), shape(ffn, hidden)],
        scratch_shapes=[vmem(seq, hidden), vmem(*w.shape), vmem(chips, m, 2 * rows), vmem(seq, ffn), vmem(seq, hidden),
                        vmem(2, seq, unit), vmem(2, seq, unit), vmem(unit, seq), vmem(2, unit, ffn), vmem(2, unit, hidden),
                        dma((13,)), dma((13,)), dma((4,)), dma((chips,)), dma((chips,)),
                        dma((2,)), dma((2,)), dma((2,)), dma((2,))],
        compiler_params=pltpu.CompilerParams(collective_id=cid, has_side_effects=True, vmem_limit_bytes=60 * 2 ** 20),
        cost_estimate=pl.CostEstimate(flops=60 * 10 ** 9, bytes_accessed=6 * seq * hidden, transcendentals=0),
        name="gather_grads",
    )(x, w, b1, dz, g, dy)


def add_rows(dst, start, count, *terms):
    step = 32

    def body(i, c):
        at = rows_at(start + i * step, step)
        total = dst[at, :].astype(jnp.float32)
        for ref, first in terms:
            total = total + ref[rows_at(first + i * step, step), :].astype(jnp.float32)
        dst[at, :] = total.astype(jnp.bfloat16)
        return c

    lax.fori_loop(0, count // step, body, 0)


class Scatter:
    def __init__(self, ring, part, pin, mid, fin, send, recv):
        self.ring, self.part, self.pin, self.mid, self.fin, self.send, self.recv = ring, part, pin, mid, fin, send, recv
        self.rows = part.shape[1] // 2
        self.half = self.rows // 2
        self.own = ring.core * self.rows

    def copy(self, k):
        r, h = self.ring, self.half
        if k < 4:
            src, dst, dev = self.part.at[k, rows_at((1 - r.core) * self.rows, self.rows)], self.pin.at[k], r.partner
        else:
            d, half, dst, dev = {4: (2, 0, self.mid.at[0], r.next), 5: (2, 1, self.mid.at[1], r.prev),
                                 6: (1, 1, self.fin.at[0, h:], r.next), 7: (1, 0, self.fin.at[0, :h], r.next),
                                 8: (3, 0, self.fin.at[1, :h], r.prev), 9: (3, 1, self.fin.at[1, h:], r.prev)}[k]
            src = self.part.at[d, rows_at(self.own + half * h, h)]
        return pltpu.make_async_remote_copy(src_ref=src, dst_ref=dst, send_sem=self.send.at[k], recv_sem=self.recv.at[k],
                                            device_id={'model': dev}, device_id_type=MESH)

    def start(self, k):
        self.copy(k).start()

    def arrived(self, k):
        self.copy(k).wait_recv()

    def join(self, d):
        self.arrived(d)
        add_rows(self.part.at[d], self.own, self.rows, (self.pin.at[d], 0))

    def run(self, product, filler, out_ref):
        h = self.half
        product(2)
        self.start(2)
        product(1)
        self.start(1)
        self.join(2)
        self.start(4)
        self.start(5)
        product(3)
        self.start(3)
        self.join(1)
        self.start(6)
        self.join(3)
        self.start(8)
        product(0)
        self.start(0)
        self.join(0)
        self.arrived(4)
        add_rows(self.part.at[1], self.own, h, (self.mid.at[0], 0))
        self.start(7)
        self.arrived(5)
        add_rows(self.part.at[3], self.own + h, h, (self.mid.at[1], 0))
        self.start(9)
        filler()
        for k in (6, 7, 8, 9):
            self.arrived(k)
        step = 32

        def body(i, c):
            at = rows_at(i * step, step)
            total = self.part[0, rows_at(self.own + i * step, step), :].astype(jnp.float32)
            total = total + self.fin[0, at, :].astype(jnp.float32) + self.fin[1, at, :].astype(jnp.float32)
            out_ref[at, :] = total.astype(jnp.bfloat16)
            return c

        lax.fori_loop(0, self.rows // step, body, 0)
        for k in range(10):
            self.copy(k).wait_send()


def scatter_scratch(rows, hidden, dtype):
    dma = pltpu.SemaphoreType.DMA
    return [pltpu.VMEM((4, 2 * rows, hidden), dtype), pltpu.VMEM((4, rows, hidden), dtype),
            pltpu.VMEM((2, rows // 2, hidden), dtype), pltpu.VMEM((2, rows, hidden), dtype), dma((10,)), dma((10,))]


def scatter_t_kernel(n, tile, x_ref, w_ref, out_ref, x_s, w_s, lhs, part, pin, mid, fin, send, recv, load):
    ring = Ring(n)
    cx = pltpu.make_async_copy(x_ref, x_s, load.at[0])
    cx.start()
    cw = pltpu.make_async_copy(w_ref, w_s, load.at[1])
    cw.start()
    ring.barrier()
    cx.wait()
    cw.wait()
    sc = Scatter(ring, part, pin, mid, fin, send, recv)
    wide = part.shape[1]

    def product(d):
        at = rows_at(ring.ahead(d) * wide, wide)
        lhs[...] = x_s[:, at].T

        def body(t, c):
            cols = rows_at(t * tile, tile)
            part[d, :, cols] = dot32(lhs[...], w_s[:, cols]).astype(jnp.bfloat16)
            return c

        lax.fori_loop(0, w_s.shape[1] // tile, body, 0)

    sc.run(product, lambda: None, out_ref)


def scatter_t(n, cid, x, w, tile=512):
    (m, seq), hidden = x.shape, w.shape[1]
    rows = seq // n
    dma = pltpu.SemaphoreType.DMA
    return pl.pallas_call(
        functools.partial(scatter_t_kernel, n, tile),
        in_specs=[pl.BlockSpec(memory_space=pl.ANY)] * 2,
        out_specs=pl.BlockSpec(memory_space=pltpu.VMEM),
        out_shape=jax.ShapeDtypeStruct((rows, hidden), x.dtype),
        scratch_shapes=[pltpu.VMEM(x.shape, x.dtype), pltpu.VMEM(w.shape, x.dtype), pltpu.VMEM((2 * rows, m), x.dtype)]
        + scatter_scratch(rows, hidden, x.dtype) + [dma((2,))],
        compiler_params=pltpu.CompilerParams(collective_id=cid, has_side_effects=True, vmem_limit_bytes=60 * 2 ** 20),
        cost_estimate=pl.CostEstimate(flops=40 * 10 ** 9, bytes_accessed=3 * seq * hidden, transcendentals=0),
        name="scatter_t",
    )(x, w)


def scatter_grads_kernel(n, tile, x_ref, w_ref, a_ref, o_ref, d_ref, out_ref, gq_ref, go_ref,
                         x_s, w_s, lhs, o_s, a_s, d_s, gq_st, go_st, part, pin, mid, fin, send, recv, load, a_l, a_p, d_l, d_p):
    ring = Ring(n)
    loads = [pltpu.make_async_copy(a, b, load.at[i]) for i, (a, b) in enumerate(((x_ref, x_s), (w_ref, w_s), (o_ref, o_s)))]
    for cp in loads:
        cp.start()
    wq = Product(a_ref, x_s, gq_ref, a_s, gq_st, a_l, a_p, False)
    wo = Product(d_ref, o_s, go_ref, d_s, go_st, d_l, d_p, False)
    wq.get(0).start()
    wo.get(0).start()
    ring.barrier()
    loads[0].wait()
    loads[1].wait()
    sc = Scatter(ring, part, pin, mid, fin, send, recv)
    wide = part.shape[1]

    def product(d):
        at = rows_at(ring.ahead(d) * wide, wide)
        lhs[...] = x_s[:, at].T

        def body(t, c):
            cols = rows_at(t * tile, tile)
            part[d, :, cols] = dot32(lhs[...], w_s[:, cols]).astype(jnp.bfloat16)
            return c

        lax.fori_loop(0, w_s.shape[1] // tile, body, 0)

    def filler():
        loads[2].wait()
        wq.run(0, wq.total)
        wo.run(0, wo.total)

    sc.run(product, filler, out_ref)
    wq.finish()
    wo.finish()


def scatter_grads(n, cid, x, w, a, o, d, tile=512):
    (m, seq), hidden = x.shape, w.shape[1]
    rows = seq // n
    dma = pltpu.SemaphoreType.DMA
    vmem = lambda *s: pltpu.VMEM(s, x.dtype)
    any_spec = pl.BlockSpec(memory_space=pl.ANY)
    return pl.pallas_call(
        functools.partial(scatter_grads_kernel, n, tile),
        in_specs=[any_spec] * 5,
        out_specs=[pl.BlockSpec(memory_space=pltpu.VMEM), any_spec, any_spec],
        out_shape=[jax.ShapeDtypeStruct((rows, hidden), x.dtype), jax.ShapeDtypeStruct(w.shape, x.dtype),
                   jax.ShapeDtypeStruct((o.shape[0], hidden), x.dtype)],
        scratch_shapes=[vmem(*x.shape), vmem(*w.shape), vmem(2 * rows, m), vmem(*o.shape), vmem(2, seq, tile), vmem(2, seq, tile),
                        vmem(2, m, tile), vmem(2, o.shape[0], tile)]
        + scatter_scratch(rows, hidden, x.dtype) + [dma((3,)), dma((2,)), dma((2,)), dma((2,)), dma((2,))],
        compiler_params=pltpu.CompilerParams(collective_id=cid, has_side_effects=True, vmem_limit_bytes=60 * 2 ** 20),
        cost_estimate=pl.CostEstimate(flops=60 * 10 ** 9, bytes_accessed=6 * seq * hidden, transcendentals=0),
        name="scatter_grads",
    )(x, w, a, o, d)


def scatter_mlp_kernel(n, tile, dz_ref, up_ref, g_ref, down_ref, out_ref, y_ref,
                       dz_s, w_s, g_s, down_s, part, pin, mid, fin, send, recv, load, ystage, put):
    ring = Ring(n)
    loads = [pltpu.make_async_copy(a, b, load.at[i]) for i, (a, b) in
             enumerate(((dz_ref, dz_s), (up_ref, w_s), (g_ref, g_s), (down_ref, down_s)))]
    for cp in loads:
        cp.start()
    ring.barrier()
    loads[0].wait()
    loads[1].wait()
    sc = Scatter(ring, part, pin, mid, fin, send, recv)
    wide = part.shape[1]
    hidden = part.shape[2]

    def product(d):
        at = rows_at(ring.ahead(d) * wide, wide)

        def body(t, c):
            cols = rows_at(t * tile, tile)
            part[d, :, cols] = dot_nt(dz_s[at, :], w_s[cols, :]).astype(jnp.bfloat16)
            return c

        lax.fori_loop(0, hidden // tile, body, 0)

    def filler():
        loads[2].wait()
        loads[3].wait()
        puts = []
        for q in range(n // 2):
            if q >= 2:
                puts[q - 2].wait()

            def body(t, c):
                cols = rows_at(t * tile, tile)
                ystage[q % 2, :, cols] = dot32(g_s[q * wide:(q + 1) * wide, :], down_s[:, cols]).astype(jnp.bfloat16)
                return c

            lax.fori_loop(0, hidden // tile, body, 0)
            puts.append(pltpu.make_async_copy(ystage.at[q % 2], y_ref.at[q * wide:(q + 1) * wide], put.at[q]))
            puts[q].start()
        for cp in puts[-2:]:
            cp.wait()

    sc.run(product, filler, out_ref)


def scatter_mlp(n, cid, dz, up, g, down, tile=512):
    (seq, ffn), hidden = dz.shape, down.shape[1]
    rows = seq // n
    dma = pltpu.SemaphoreType.DMA
    return pl.pallas_call(
        functools.partial(scatter_mlp_kernel, n, tile),
        in_specs=[pl.BlockSpec(memory_space=pl.ANY)] * 4,
        out_specs=[pl.BlockSpec(memory_space=pltpu.VMEM), pl.BlockSpec(memory_space=pl.ANY)],
        out_shape=[jax.ShapeDtypeStruct((rows, hidden), dz.dtype), jax.ShapeDtypeStruct((seq, hidden), dz.dtype)],
        scratch_shapes=[pltpu.VMEM(a.shape, a.dtype) for a in (dz, up, g, down)]
        + scatter_scratch(rows, hidden, dz.dtype) + [dma((4,)), pltpu.VMEM((2, 2 * rows, hidden), dz.dtype), dma((n // 2,))],
        compiler_params=pltpu.CompilerParams(collective_id=cid, has_side_effects=True, vmem_limit_bytes=63 * 2 ** 20),
        cost_estimate=pl.CostEstimate(flops=60 * 10 ** 9, bytes_accessed=3 * seq * hidden, transcendentals=0),
        name="scatter_mlp",
    )(dz, up, g, down)


def group_sum_kernel(n, x_ref, out_ref, slots, send, recv):
    me = lax.axis_index('model')
    sem = pltpu.get_barrier_semaphore()
    peers = [lax.rem(me + k, n) for k in range(1, n)]
    for dev in peers:
        pl.semaphore_signal(sem, inc=1, device_id={'model': dev}, device_id_type=MESH)
    pl.semaphore_wait(sem, n - 1)
    copies = [pltpu.make_async_remote_copy(src_ref=x_ref, dst_ref=slots.at[me], send_sem=send.at[k], recv_sem=recv.at[k],
                                           device_id={'model': dev}, device_id_type=MESH) for k, dev in enumerate(peers)]
    for cp in copies:
        cp.start()
    slots[me] = x_ref[...]
    for cp in copies:
        cp.wait()
    total = slots[0]
    for k in range(1, n):
        total = total + slots[k]
    out_ref[...] = total.astype(out_ref.dtype)


def group_sum(vals, n, cid):
    dma = pltpu.SemaphoreType.DMA
    return pl.pallas_call(
        functools.partial(group_sum_kernel, n),
        in_specs=[pl.BlockSpec(memory_space=pltpu.VMEM)],
        out_specs=pl.BlockSpec(memory_space=pltpu.VMEM),
        out_shape=jax.ShapeDtypeStruct(vals.shape, jnp.bfloat16),
        scratch_shapes=[pltpu.VMEM((n,) + vals.shape, vals.dtype), dma((n - 1,)), dma((n - 1,))],
        compiler_params=pltpu.CompilerParams(collective_id=cid, has_side_effects=True),
        cost_estimate=pl.CostEstimate(flops=10 ** 9, bytes_accessed=vals.size * 4, transcendentals=0),
        name="group_sum",
    )(vals)


def local_layer(n, hidden_in, seg_ids, gain_attn, w_qkv, w_out, gain_mlp, w_up, w_down, grad_out):
    heads, hd, hidden = w_out.shape
    seq_len = seg_ids.shape[1]
    x_f32 = hidden_in[0].astype(jnp.float32)
    dy = grad_out[0]
    wq_t = jnp.transpose(w_qkv, (1, 2, 3, 0)).reshape(heads * 3 * hd, hidden)
    wo = w_out.reshape(heads * hd, hidden)
    first = jnp.sum(seg_ids[0][:, None] < seg_ids[0][None, :], axis=0, dtype=jnp.int32)
    lo = first[::BLK] // BLK
    first = first[None]
    gather = lambda a: lax.all_gather(a, 'model', axis=0, tiled=True)
    scatter = lambda a: lax.psum_scatter(a, 'model', scatter_dimension=0, tiled=True)

    ln1_out, ln1_vjp = jax.vjp(layer_norm, x_f32, gain_attn.astype(jnp.float32))
    attn_in, qkv_t = gather_t(n, 0, ln1_out.astype(jnp.bfloat16), wq_t, 320)
    dy_late, qkv_t = lax.optimization_barrier((dy, qkv_t))
    grad_full = gather(dy_late)
    o_t, lse = attention_fwd(qkv_t, lo, first, heads, hd)
    attn_sum = scatter_t(n, 1, o_t, wo)
    mid_loc = (x_f32 + attn_sum.astype(jnp.float32)).astype(jnp.bfloat16)
    ln2_out, ln2_vjp = jax.vjp(layer_norm, mid_loc.astype(jnp.float32), gain_mlp.astype(jnp.float32))
    mlp_in, act_lo, d_pre = mlp(n, 2, ln2_out.astype(jnp.bfloat16), grad_full, w_up, w_down)
    d_mlp_in, mlp_part = scatter_mlp(n, 3, d_pre, w_up, act_lo, w_down)
    d_mid_ln, d_gain_mlp = ln2_vjp(d_mlp_in.astype(jnp.float32))
    d_mid = (dy.astype(jnp.float32) + d_mid_ln).astype(jnp.bfloat16)
    d_mid_full, do_t, g_up, g_down = gather_grads(n, 4, d_mid, wo, mlp_in, d_pre, act_lo, grad_full)
    mlp_part, do_t = lax.optimization_barrier((mlp_part, do_t))
    mlp_sum = scatter(mlp_part)
    hidden_out = (mid_loc.astype(jnp.float32) + mlp_sum.astype(jnp.float32)).astype(jnp.bfloat16)
    dqkv_t = attention_bwd(qkv_t, o_t, do_t, lse, lo, first, heads, hd)
    d_attn_in, g_qkv, g_out = scatter_grads(n, 5, dqkv_t, wq_t, attn_in, o_t, d_mid_full)
    d_x_ln, d_gain_attn = ln1_vjp(d_attn_in.astype(jnp.float32))
    grad_in = (d_mid.astype(jnp.float32) + d_x_ln).astype(jnp.bfloat16)
    gain_sums = group_sum(jnp.stack([d_gain_attn, d_gain_mlp]), n, 6)
    g_qkv = jnp.transpose(g_qkv.reshape(heads, 3, hd, hidden), (3, 0, 1, 2))
    return (hidden_out[None], grad_in[None], g_qkv, g_out.reshape(heads, hd, hidden), g_up, g_down,
            gain_sums[0], gain_sums[1])


def solution(mesh):
    act_spec = P('data', 'model', None)
    in_specs = (act_spec, P('data', None), P(), P(None, 'model', None, None), P('model', None, None), P(), P(None, 'model'), P('model', None), act_spec)
    out_specs = (act_spec, act_spec, P('data', 'model', None, None), P(('data', 'model'), None, None), P('data', 'model'), P(('data', 'model'), None), P('data'), P('data'))
    return jax.shard_map(functools.partial(local_layer, mesh.shape['model']), mesh=mesh, in_specs=in_specs, out_specs=out_specs, check_vma=False)
```

```python
import functools

import jax
import jax.numpy as jnp
from jax import lax
from jax.experimental import pallas as pl
from jax.experimental.pallas import tpu as pltpu
from jax.sharding import PartitionSpec as P

LN_EPS = 1e-5
BLK = 256
NT = (((1,), (1,)), ((), ()))
MESH = pl.DeviceIdType.MESH


def layer_norm(x_f32, gain_f32):
    mean_val = jnp.mean(x_f32, axis=-1, keepdims=True)
    centered = x_f32 - mean_val
    variance = jnp.mean(centered * centered, axis=-1, keepdims=True)
    return centered * lax.rsqrt(variance + LN_EPS) * gain_f32


def gelu_tanh(pre_act):
    return jax.nn.gelu(pre_act, approximate=True)


def dot32(a, b):
    return jnp.dot(a, b, preferred_element_type=jnp.float32)


def visible(j, i, first_row):
    kpos = j * BLK + lax.broadcasted_iota(jnp.int32, (BLK, BLK), 0)
    qpos = i * BLK + lax.broadcasted_iota(jnp.int32, (BLK, BLK), 1)
    return (kpos <= qpos) & (kpos >= first_row)


def attn_fwd_kernel(heads, hd, lo_ref, qkv_ref, first_ref, o_ref, lse_ref, k_s, s_s, o_s):
    i = pl.program_id(0)
    scale = hd ** -0.5

    @pl.when(i == 0)
    def _():
        for h in range(heads):
            for j in range(k_s.shape[1] // BLK):
                kt = qkv_ref[(3 * h + 1) * hd:(3 * h + 2) * hd, j * BLK:(j + 1) * BLK]
                k_s[h, j * BLK:(j + 1) * BLK, :] = kt.T

    lo = lo_ref[i]
    cols = pl.ds(pl.multiple_of(i * BLK, BLK), BLK)
    first_row = first_ref[0:1, cols]
    neg = jnp.full((8, BLK), -jnp.inf, jnp.float32)

    def scores(j, m):
        rows = pl.ds(pl.multiple_of(j * BLK, BLK), BLK)
        mask = visible(j, i, first_row)
        out = []
        for h in range(heads):
            s = dot32(k_s[h, rows, :], qkv_ref[3 * h * hd:(3 * h + 1) * hd, cols]) * scale
            s = jnp.where(mask, s, -1e30)
            s_s[h, rows, :] = s
            out.append(jnp.maximum(m[h], jnp.max(s.reshape(BLK // 8, 8, BLK), axis=0)))
        return tuple(out)

    m = lax.fori_loop(lo, i + 1, scores, (neg,) * heads)
    m = [jnp.max(x, axis=0, keepdims=True) for x in m]

    def expo(j, l):
        rows = pl.ds(pl.multiple_of(j * BLK, BLK), BLK)
        out = []
        for h in range(heads):
            e = jnp.exp(s_s[h, rows, :] - m[h])
            s_s[h, rows, :] = e
            out.append(l[h] + jnp.sum(e.reshape(BLK // 8, 8, BLK), axis=0))
        return tuple(out)

    l = lax.fori_loop(lo, i + 1, expo, (jnp.zeros((8, BLK), jnp.float32),) * heads)
    l = [jnp.sum(x, axis=0, keepdims=True) for x in l]
    r = [1.0 / x for x in l]
    for h in range(heads):
        lse_ref[h:h + 1, :] = m[h] + jnp.log(l[h])
        o_s[h] = jnp.zeros((hd, BLK), jnp.float32)

    def values(j, c):
        rows = pl.ds(pl.multiple_of(j * BLK, BLK), BLK)
        for h in range(heads):
            pb = (s_s[h, rows, :] * r[h]).astype(jnp.bfloat16)
            o_s[h] += dot32(qkv_ref[(3 * h + 2) * hd:(3 * h + 3) * hd, rows], pb)
        return c

    lax.fori_loop(lo, i + 1, values, 0)
    for h in range(heads):
        o_ref[h * hd:(h + 1) * hd, :] = o_s[h].astype(jnp.bfloat16)


def attention_fwd(qkv_t, lo, first, heads, hd):
    seq = qkv_t.shape[1]
    nb = seq // BLK
    flops = 4 * heads * seq * seq * hd // 2
    return pl.pallas_call(
        functools.partial(attn_fwd_kernel, heads, hd),
        grid_spec=pltpu.PrefetchScalarGridSpec(
            num_scalar_prefetch=1, grid=(nb,),
            in_specs=[pl.BlockSpec(qkv_t.shape, lambda i, lo: (0, 0)),
                      pl.BlockSpec((1, seq), lambda i, lo: (0, 0))],
            out_specs=[pl.BlockSpec((heads * hd, BLK), lambda i, lo: (0, i)),
                       pl.BlockSpec((8, BLK), lambda i, lo: (0, i))],
            scratch_shapes=[pltpu.VMEM((heads, seq, hd), jnp.bfloat16),
                            pltpu.VMEM((heads, seq, BLK), jnp.float32),
                            pltpu.VMEM((heads, hd, BLK), jnp.float32)]),
        out_shape=[jax.ShapeDtypeStruct((heads * hd, seq), jnp.bfloat16),
                   jax.ShapeDtypeStruct((8, seq), jnp.float32)],
        compiler_params=pltpu.CompilerParams(vmem_limit_bytes=56 * 2 ** 20),
        cost_estimate=pl.CostEstimate(flops=8 * flops, bytes_accessed=2 * qkv_t.size, transcendentals=0),
        name="attn_fwd",
    )(lo, qkv_t, first)


def attn_bwd_kernel(heads, hd, lo_ref, qkv_ref, o_ref, do_ref, lse_ref, first_ref, up_ref, down_ref, d_ref, up_out, down_out,
                    k_s, v_s, dq_s, dk_s, dv_s):
    i = pl.program_id(0)
    seq = qkv_ref.shape[1]
    scale = hd ** -0.5

    @pl.when(i == 0)
    def _():
        dk_s[...] = jnp.zeros_like(dk_s)
        dv_s[...] = jnp.zeros_like(dv_s)
        for h in range(heads):
            for j in range(seq // BLK):
                c = slice(j * BLK, (j + 1) * BLK)
                k_s[h, c, :] = qkv_ref[(3 * h + 1) * hd:(3 * h + 2) * hd, c].T
                v_s[h, c, :] = qkv_ref[(3 * h + 2) * hd:(3 * h + 3) * hd, c].T

    up_out[...] = up_ref[...]
    down_out[...] = down_ref[...]
    lo = lo_ref[i]
    cols = pl.ds(pl.multiple_of(i * BLK, BLK), BLK)
    first_row = first_ref[0:1, cols]
    delta = []
    for h in range(heads):
        hs = slice(h * hd, (h + 1) * hd)
        delta.append(jnp.sum(do_ref[hs, :].astype(jnp.float32) * o_ref[hs, :].astype(jnp.float32), axis=0, keepdims=True))
        dq_s[h] = jnp.zeros((hd, BLK), jnp.float32)

    def step(j, c):
        rows = pl.ds(pl.multiple_of(j * BLK, BLK), BLK)
        mask = visible(j, i, first_row)
        for h in range(heads):
            q_t = qkv_ref[3 * h * hd:(3 * h + 1) * hd, cols]
            do_t = do_ref[h * hd:(h + 1) * hd, :]
            s = dot32(k_s[h, rows, :], q_t) * scale
            p = jnp.exp(jnp.where(mask, s, -1e30) - lse_ref[h:h + 1, :])
            dp = dot32(v_s[h, rows, :], do_t)
            ds = (p * (dp - delta[h]) * scale).astype(jnp.bfloat16)
            pb = p.astype(jnp.bfloat16)
            dq_s[h] += dot32(qkv_ref[(3 * h + 1) * hd:(3 * h + 2) * hd, rows], ds)
            dk_s[h, :, rows] += lax.dot_general(q_t, ds, NT, preferred_element_type=jnp.float32)
            dv_s[h, :, rows] += lax.dot_general(do_t, pb, NT, preferred_element_type=jnp.float32)
        return c

    lax.fori_loop(lo, i + 1, step, 0)
    for h in range(heads):
        d_ref[3 * h * hd:(3 * h + 1) * hd, cols] = dq_s[h].astype(jnp.bfloat16)

    @pl.when(i == pl.num_programs(0) - 1)
    def _():
        for h in range(heads):
            d_ref[(3 * h + 1) * hd:(3 * h + 2) * hd, :] = dk_s[h].astype(jnp.bfloat16)
            d_ref[(3 * h + 2) * hd:(3 * h + 3) * hd, :] = dv_s[h].astype(jnp.bfloat16)


def attention_bwd(qkv_t, o_t, do_t, lse, lo, first, g_up, g_down, heads, hd):
    seq = qkv_t.shape[1]
    nb = seq // BLK
    flops = 10 * heads * seq * seq * hd // 2
    blk = lambda rows: pl.BlockSpec((rows, BLK), lambda i, lo: (0, i))
    through = [pl.BlockSpec((a.shape[0] // nb, a.shape[1]), lambda i, lo: (i, 0)) for a in (g_up, g_down)]
    return pl.pallas_call(
        functools.partial(attn_bwd_kernel, heads, hd),
        grid_spec=pltpu.PrefetchScalarGridSpec(
            num_scalar_prefetch=1, grid=(nb,),
            in_specs=[pl.BlockSpec(qkv_t.shape, lambda i, lo: (0, 0)), blk(heads * hd), blk(heads * hd), blk(8),
                      pl.BlockSpec((1, seq), lambda i, lo: (0, 0))] + through,
            out_specs=[pl.BlockSpec(qkv_t.shape, lambda i, lo: (0, 0))] + through,
            scratch_shapes=[pltpu.VMEM((heads, seq, hd), jnp.bfloat16),
                            pltpu.VMEM((heads, seq, hd), jnp.bfloat16),
                            pltpu.VMEM((heads, hd, BLK), jnp.float32),
                            pltpu.VMEM((heads, hd, seq), jnp.float32),
                            pltpu.VMEM((heads, hd, seq), jnp.float32)]),
        out_shape=[jax.ShapeDtypeStruct(a.shape, jnp.bfloat16) for a in (qkv_t, g_up, g_down)],
        compiler_params=pltpu.CompilerParams(vmem_limit_bytes=56 * 2 ** 20),
        cost_estimate=pl.CostEstimate(flops=8 * flops, bytes_accessed=4 * qkv_t.size, transcendentals=0),
        name="attn_bwd",
    )(lo, qkv_t, o_t, do_t, lse, first, g_up, g_down)


def dot_nt(a, b):
    return lax.dot_general(a, b, NT, preferred_element_type=jnp.float32)


class Ring:
    def __init__(self, n):
        self.n = n
        self.me = lax.axis_index('model')
        self.core = lax.rem(self.me, 2)
        self.chip = self.me // 2
        self.partner = self.me + 1 - 2 * self.core
        self.next = lax.rem(self.me + 2, n)
        self.prev = lax.rem(self.me + n - 2, n)
        self.opp = lax.rem(self.me + n // 2, n)

    def barrier(self, peers=None):
        sem = pltpu.get_barrier_semaphore()
        peers = peers or (self.partner, self.next, self.prev)
        for dev in peers:
            pl.semaphore_signal(sem, inc=1, device_id={'model': dev}, device_id_type=MESH)
        pl.semaphore_wait(sem, len(peers))

    def ahead(self, d):
        return lax.rem(self.chip + d, self.n // 2)


def rows_at(start, size, unit=None):
    return pl.ds(pl.multiple_of(start, unit or size), size)


class Gather:
    def __init__(self, ring, buf, send, recv):
        self.ring, self.buf, self.send, self.recv = ring, buf, send, recv
        self.rows = buf.shape[0] // ring.n
        self.half = self.rows // 2
        r = ring
        self.table = {0: (r.me, None, r.partner),
                      1: (r.me, 0, r.next), 2: (r.me, 1, r.next), 3: (r.prev, 0, r.next),
                      4: (r.me, 1, r.prev), 5: (r.me, 0, r.prev), 6: (r.next, 1, r.prev),
                      7: (r.prev, 0, r.partner), 8: (r.prev, 1, r.partner),
                      9: (r.next, 1, r.partner), 10: (r.next, 0, r.partner),
                      11: (r.opp, 0, r.partner), 12: (r.opp, 1, r.partner)}

    def copy(self, k):
        owner, part, dev = self.table[k]
        if part is None:
            ref = self.buf.at[rows_at(owner * self.rows, self.rows)]
        else:
            ref = self.buf.at[rows_at(owner * self.rows + part * self.half, self.half)]
        return pltpu.make_async_remote_copy(src_ref=ref, dst_ref=ref, send_sem=self.send.at[k], recv_sem=self.recv.at[k],
                                            device_id={'model': dev}, device_id_type=MESH)

    def start(self, *ks):
        for k in ks:
            self.copy(k).start()

    def arrived(self, *ks):
        for k in ks:
            self.copy(k).wait_recv()

    def run(self, compute, fill=lambda k: None):
        self.start(1, 4, 0, 2, 5)
        self.arrived(0)
        compute(self.ring.chip)
        fill(0)
        self.arrived(1)
        self.start(3, 7)
        self.arrived(4)
        self.start(6, 9)
        fill(1)
        self.arrived(2)
        self.start(8)
        self.arrived(5)
        self.start(10)
        self.arrived(7, 8)
        compute(self.ring.ahead(self.ring.n // 2 - 1))
        self.arrived(9, 10)
        compute(self.ring.ahead(1))
        fill(2)
        self.arrived(3)
        self.start(11)
        self.arrived(6)
        self.start(12)
        self.arrived(11, 12)
        compute(self.ring.ahead(self.ring.n // 4))
        for k in self.table:
            self.copy(k).wait_send()


def gather_t_kernel(n, tile, x_ref, w_ref, full_ref, out_ref, buf, w_s, stage, send, recv, load, store, put):
    ring = Ring(n)
    rows = x_ref.shape[0]
    mine = pltpu.make_async_copy(x_ref, buf.at[rows_at(ring.me * rows, rows)], load.at[0])
    mine.start()
    weights = pltpu.make_async_copy(w_ref, w_s, load.at[1])
    weights.start()
    ring.barrier()
    mine.wait()
    g = Gather(ring, buf, send, recv)
    pending = []

    def compute(chip):
        s = len(pending)
        if s == 0:
            weights.wait()
        at = rows_at(chip * (2 * rows), 2 * rows)
        keep = pltpu.make_async_copy(buf.at[at], full_ref.at[at], store.at[s])
        keep.start()

        def body(t, c):
            w_rows = rows_at(t * tile, tile)
            stage[s, w_rows, :] = dot_nt(w_s[w_rows, :], buf[at, :]).astype(jnp.bfloat16)
            return c

        lax.fori_loop(0, w_s.shape[0] // tile, body, 0)
        out = pltpu.make_async_copy(stage.at[s], out_ref.at[:, at], put.at[s])
        out.start()
        pending.append((keep, out))

    g.run(compute)
    for pair in pending:
        for cp in pair:
            cp.wait()


def gather_t(n, cid, x, w, tile):
    rows, hidden = x.shape
    seq, m, chips = rows * n, w.shape[0], n // 2
    dma = pltpu.SemaphoreType.DMA
    return pl.pallas_call(
        functools.partial(gather_t_kernel, n, tile),
        in_specs=[pl.BlockSpec(memory_space=pl.ANY)] * 2,
        out_specs=[pl.BlockSpec(memory_space=pl.ANY)] * 2,
        out_shape=[jax.ShapeDtypeStruct((seq, hidden), x.dtype), jax.ShapeDtypeStruct((m, seq), x.dtype)],
        scratch_shapes=[pltpu.VMEM((seq, hidden), x.dtype), pltpu.VMEM(w.shape, w.dtype),
                        pltpu.VMEM((chips, m, 2 * rows), x.dtype),
                        dma((13,)), dma((13,)), dma((2,)), dma((chips,)), dma((chips,))],
        compiler_params=pltpu.CompilerParams(collective_id=cid, has_side_effects=True, vmem_limit_bytes=60 * 2 ** 20),
        cost_estimate=pl.CostEstimate(flops=40 * 10 ** 9, bytes_accessed=3 * seq * hidden, transcendentals=0),
        name="gather_t",
    )(x, w)


def mlp_kernel(n, tile, x_ref, dy_ref, up_ref, down_ref, full_ref, g_ref, dz_ref,
               buf, dy_s, up_s, down_s, g_s, dz_s, da_s, send, recv, load, store, put, put2, dy_sem):
    ring = Ring(n)
    rows = x_ref.shape[0]
    mine = pltpu.make_async_copy(x_ref, buf.at[rows_at(ring.me * rows, rows)], load.at[0])
    mine.start()
    w_up = pltpu.make_async_copy(up_ref, up_s, load.at[1])
    w_up.start()
    w_down = pltpu.make_async_copy(down_ref, down_s, load.at[2])
    w_down.start()
    order = [ring.chip, ring.ahead(n // 2 - 1), ring.ahead(1), ring.ahead(n // 4)]

    def dy_copy(s):
        return pltpu.make_async_copy(dy_ref.at[rows_at(order[s] * (2 * rows), 2 * rows)], dy_s.at[s % 2], dy_sem.at[s])

    dy_copy(0).start()
    dy_copy(1).start()
    ring.barrier()
    mine.wait()
    g = Gather(ring, buf, send, recv)
    pending = []
    root = (2.0 / jnp.pi) ** 0.5

    def compute(chip):
        s = len(pending)
        if s == 0:
            w_up.wait()
            w_down.wait()
        at = rows_at(chip * (2 * rows), 2 * rows)
        keep = pltpu.make_async_copy(buf.at[at], full_ref.at[at], store.at[s])
        keep.start()
        if s >= 2:
            for cp in pending[s - 2][1:]:
                cp.wait()
        if s == 0:
            dy_copy(0).wait()

        def body(t, c):
            cols = rows_at(t * tile, tile)
            z = dot32(buf[at, :], up_s[:, cols])
            if s == 0:
                da = dot_nt(dy_s[0], down_s[cols, :])
            else:
                da = da_s[s - 1, :, cols]
            z2 = z * z
            th = jnp.tanh(root * (z + 0.044715 * (z2 * z)))
            cdf = 0.5 * (1.0 + th)
            g_s[s % 2, :, cols] = (z * cdf).astype(jnp.bfloat16)
            slope = cdf + (0.5 * z) * (1.0 - th * th) * (root * (1.0 + (3 * 0.044715) * z2))
            dz_s[s % 2, :, cols] = (slope * da).astype(jnp.bfloat16)
            return c

        lax.fori_loop(0, up_s.shape[1] // tile, body, 0)
        if s == 0:
            dy_copy(2).start()
        og = pltpu.make_async_copy(g_s.at[s % 2], g_ref.at[at], put.at[s])
        od = pltpu.make_async_copy(dz_s.at[s % 2], dz_ref.at[at], put2.at[s])
        og.start()
        od.start()
        pending.append((keep, og, od))

    def fill(k):
        if k == 1:
            for s in range(1, n // 2):
                dy_copy(s).wait()

                def body(t, c):
                    cols = rows_at(t * tile, tile)
                    da_s[s - 1, :, cols] = dot_nt(dy_s[s % 2], down_s[cols, :])
                    return c

                lax.fori_loop(0, up_s.shape[1] // tile, body, 0)
                if s + 2 < n // 2:
                    dy_copy(s + 2).start()

    g.run(compute, fill)
    for s, cps in enumerate(pending):
        for cp in (cps if s >= n // 2 - 2 else cps[:1]):
            cp.wait()


def mlp(n, cid, x, dy, up, down, tile=256):
    rows, hidden = x.shape
    seq, ffn, chips = rows * n, up.shape[1], n // 2
    dma = pltpu.SemaphoreType.DMA
    return pl.pallas_call(
        functools.partial(mlp_kernel, n, tile),
        in_specs=[pl.BlockSpec(memory_space=pl.ANY)] * 4,
        out_specs=[pl.BlockSpec(memory_space=pl.ANY)] * 3,
        out_shape=[jax.ShapeDtypeStruct((seq, hidden), x.dtype)] + [jax.ShapeDtypeStruct((seq, ffn), x.dtype)] * 2,
        scratch_shapes=[pltpu.VMEM((seq, hidden), x.dtype), pltpu.VMEM((2, 2 * rows, hidden), x.dtype),
                        pltpu.VMEM(up.shape, x.dtype), pltpu.VMEM(down.shape, x.dtype),
                        pltpu.VMEM((2, 2 * rows, ffn), x.dtype), pltpu.VMEM((2, 2 * rows, ffn), x.dtype),
                        pltpu.VMEM((chips - 1, 2 * rows, ffn), jnp.float32),
                        dma((13,)), dma((13,)), dma((3,)), dma((chips,)), dma((chips,)), dma((chips,)), dma((chips,))],
        compiler_params=pltpu.CompilerParams(collective_id=cid, has_side_effects=True, vmem_limit_bytes=60 * 2 ** 20),
        cost_estimate=pl.CostEstimate(flops=40 * 10 ** 9, bytes_accessed=3 * seq * hidden, transcendentals=0),
        name="gather_mlp",
    )(x, dy, up, down)


class Product:
    def __init__(self, x, fixed, out, slots, stage, load, store, rows, lhs=None):
        self.x, self.fixed, self.out, self.slots, self.stage = x, fixed, out, slots, stage
        self.load, self.store, self.rows, self.lhs = load, store, rows, lhs
        self.unit = slots.shape[2]
        self.total = x.shape[1] // self.unit

    def get(self, u):
        slot = lax.rem(u, 2)
        return pltpu.make_async_copy(self.x.at[:, rows_at(u * self.unit, self.unit)], self.slots.at[slot], self.load.at[slot])

    def put(self, u):
        slot = lax.rem(u, 2)
        at = rows_at(u * self.unit, self.unit)
        dst = self.out.at[at] if self.rows else self.out.at[:, at]
        return pltpu.make_async_copy(self.stage.at[slot], dst, self.store.at[slot])

    def run(self, first, last):
        def body(u, c):
            slot = lax.rem(u, 2)
            self.get(u).wait()

            @pl.when(u + 1 < self.total)
            def _():
                self.get(u + 1).start()

            @pl.when(u >= 2)
            def _():
                self.put(u - 2).wait()

            if self.rows:
                self.lhs[...] = self.slots[slot].T
                width = self.fixed.shape[1]
                for w in range(0, width, 1280):
                    at = slice(w, min(w + 1280, width))
                    self.stage[slot, :, at] = dot32(self.lhs[...], self.fixed[:, at]).astype(jnp.bfloat16)
            else:
                step = 320

                def part(t, c):
                    at = rows_at(t * step, step)
                    self.stage[slot, at, :] = dot32(self.fixed[at, :], self.slots[slot]).astype(jnp.bfloat16)
                    return c

                lax.fori_loop(0, self.fixed.shape[0] // step, part, 0)
            self.put(u).start()
            return c

        lax.fori_loop(first, last, body, 0)

    def finish(self):
        self.put(self.total - 2).wait()
        self.put(self.total - 1).wait()


def gather_grads_kernel(n, x_ref, w_ref, b_ref, dz_ref, g_ref, dy_ref, full_ref, out_ref, up_ref, down_ref,
                        buf, w_s, stage, dz_s, dy_s, b_s, g_s, lhs, up_st, down_st,
                        send, recv, load, store, put, up_l, up_p, down_l, down_p):
    ring = Ring(n)
    rows = x_ref.shape[0]
    loads = [pltpu.make_async_copy(a, b, load.at[i]) for i, (a, b) in
             enumerate(((x_ref, buf.at[rows_at(ring.me * rows, rows)]), (w_ref, w_s), (dz_ref, dz_s), (dy_ref, dy_s)))]
    up = Product(b_ref, dz_s, up_ref, b_s, up_st, up_l, up_p, True, lhs)
    down = Product(g_ref, dy_s, down_ref, g_s, down_st, down_l, down_p, True, lhs)
    loads[0].start()
    loads[1].start()
    up.get(0).start()
    loads[2].start()
    down.get(0).start()
    loads[3].start()
    ring.barrier()
    loads[0].wait()
    g = Gather(ring, buf, send, recv)
    pending = []

    def compute(chip):
        s = len(pending)
        if s == 0:
            loads[1].wait()
        at = rows_at(chip * (2 * rows), 2 * rows)
        keep = pltpu.make_async_copy(buf.at[at], full_ref.at[at], store.at[s])
        keep.start()
        stage[s] = dot_nt(w_s[...], buf[at, :]).astype(jnp.bfloat16)
        out = pltpu.make_async_copy(stage.at[s], out_ref.at[:, at], put.at[s])
        out.start()
        pending.append((keep, out))

    def fill(k):
        mid = up.total // 2
        if k == 0:
            loads[2].wait()
            up.run(0, mid)
        elif k == 1:
            up.run(mid, up.total)
            loads[3].wait()
            down.run(0, down.total // 2)
        else:
            down.run(down.total // 2, down.total)

    g.run(compute, fill)
    up.finish()
    down.finish()
    for pair in pending:
        for cp in pair:
            cp.wait()


def gather_grads(n, cid, x, w, b1, dz, g, dy, unit=256):
    rows, hidden = x.shape
    seq, m, chips, ffn = rows * n, w.shape[0], n // 2, dz.shape[1]
    dma = pltpu.SemaphoreType.DMA
    shape = lambda *d: jax.ShapeDtypeStruct(d, x.dtype)
    vmem = lambda *d: pltpu.VMEM(d, x.dtype)
    return pl.pallas_call(
        functools.partial(gather_grads_kernel, n),
        in_specs=[pl.BlockSpec(memory_space=pl.ANY)] * 6,
        out_specs=[pl.BlockSpec(memory_space=pl.ANY)] * 4,
        out_shape=[shape(seq, hidden), shape(m, seq), shape(hidden, ffn), shape(ffn, hidden)],
        scratch_shapes=[vmem(seq, hidden), vmem(*w.shape), vmem(chips, m, 2 * rows), vmem(seq, ffn), vmem(seq, hidden),
                        vmem(2, seq, unit), vmem(2, seq, unit), vmem(unit, seq), vmem(2, unit, ffn), vmem(2, unit, hidden),
                        dma((13,)), dma((13,)), dma((4,)), dma((chips,)), dma((chips,)),
                        dma((2,)), dma((2,)), dma((2,)), dma((2,))],
        compiler_params=pltpu.CompilerParams(collective_id=cid, has_side_effects=True, vmem_limit_bytes=60 * 2 ** 20),
        cost_estimate=pl.CostEstimate(flops=60 * 10 ** 9, bytes_accessed=6 * seq * hidden, transcendentals=0),
        name="gather_grads",
    )(x, w, b1, dz, g, dy)


def add_rows(dst, start, count, *terms):
    step = 32

    def body(i, c):
        at = rows_at(start + i * step, step)
        total = dst[at, :].astype(jnp.float32)
        for ref, first in terms:
            total = total + ref[rows_at(first + i * step, step), :].astype(jnp.float32)
        dst[at, :] = total.astype(jnp.bfloat16)
        return c

    lax.fori_loop(0, count // step, body, 0)


class Scatter:
    def __init__(self, ring, part, pin, mid, fin, send, recv):
        self.ring, self.part, self.pin, self.mid, self.fin, self.send, self.recv = ring, part, pin, mid, fin, send, recv
        self.rows = part.shape[1] // 2
        self.half = self.rows // 2
        self.own = ring.core * self.rows

    def copy(self, k):
        r, h = self.ring, self.half
        if k < 4:
            src, dst, dev = self.part.at[k, rows_at((1 - r.core) * self.rows, self.rows)], self.pin.at[k], r.partner
        else:
            d, half, dst, dev = {4: (2, 0, self.mid.at[0], r.next), 5: (2, 1, self.mid.at[1], r.prev),
                                 6: (1, 1, self.fin.at[0, h:], r.next), 7: (1, 0, self.fin.at[0, :h], r.next),
                                 8: (3, 0, self.fin.at[1, :h], r.prev), 9: (3, 1, self.fin.at[1, h:], r.prev)}[k]
            src = self.part.at[d, rows_at(self.own + half * h, h)]
        return pltpu.make_async_remote_copy(src_ref=src, dst_ref=dst, send_sem=self.send.at[k], recv_sem=self.recv.at[k],
                                            device_id={'model': dev}, device_id_type=MESH)

    def start(self, k):
        self.copy(k).start()

    def arrived(self, k):
        self.copy(k).wait_recv()

    def join(self, d):
        self.arrived(d)
        add_rows(self.part.at[d], self.own, self.rows, (self.pin.at[d], 0))

    def run(self, product, filler, emit):
        h = self.half
        product(2, self.rows - self.own, self.rows, True)
        self.start(2)
        product(2, self.own, self.rows, False)
        self.join(2)
        self.start(4)
        self.start(5)
        for d in (1, 3):
            product(d, 0, 2 * self.rows, False)
            self.start(d)
        self.join(1)
        self.start(6)
        self.join(3)
        self.start(8)
        product(0, 0, 2 * self.rows, False)
        self.start(0)
        self.arrived(4)
        add_rows(self.part.at[1], self.own, h, (self.mid.at[0], 0))
        self.start(7)
        self.arrived(5)
        add_rows(self.part.at[3], self.own + h, h, (self.mid.at[1], 0))
        self.start(9)
        self.join(0)
        filler()
        for k in (6, 7, 8, 9):
            self.arrived(k)
        step = 16

        def body(i, c):
            at = rows_at(i * step, step)
            total = self.part[0, rows_at(self.own + i * step, step), :].astype(jnp.float32)
            total = total + self.fin[0, at, :].astype(jnp.float32) + self.fin[1, at, :].astype(jnp.float32)
            emit(at, total.astype(jnp.bfloat16))
            return c

        lax.fori_loop(0, self.rows // step, body, 0)
        for k in range(10):
            self.copy(k).wait_send()


def normalized(x):
    mean = jnp.mean(x, axis=-1, keepdims=True)
    cen = x - mean
    rstd = lax.rsqrt(jnp.mean(cen * cen, axis=-1, keepdims=True) + LN_EPS)
    return cen * rstd, rstd


def norm_backward(hat, rstd, gain, d):
    dh = d * gain
    return rstd * (dh - jnp.mean(dh, axis=-1, keepdims=True) - hat * jnp.mean(dh * hat, axis=-1, keepdims=True))


def fold_rows(v):
    return v[:8, :] + v[8:, :]


class Weights:
    def __init__(self, src, dst, sem, tile, rows):
        self.src, self.dst, self.sem, self.tile, self.rows = src, dst, sem, tile, rows
        self.count = src.shape[0 if rows else 1] // tile

    def copy(self, t):
        at = rows_at(t * self.tile, self.tile)
        if self.rows:
            return pltpu.make_async_copy(self.src.at[at], self.dst.at[at], self.sem.at[t])
        return pltpu.make_async_copy(self.src.at[:, at], self.dst.at[:, at], self.sem.at[t])

    def start(self):
        for t in range(self.count):
            self.copy(t).start()


def product_t(ring, tile, x_s, weights, lhs, part):
    wide = part.shape[1]

    def product(d, row0, count, first):
        if first or d != 2:
            lhs[...] = x_s[:, rows_at(ring.ahead(d) * wide, wide)].T
        at = rows_at(row0, count)

        def body(t, c):
            cols = rows_at(t * tile, tile)
            if first:
                weights.copy(t).wait()
            part[d, at, cols] = dot32(lhs[at, :], weights.dst[:, cols]).astype(jnp.bfloat16)
            return c

        lax.fori_loop(0, weights.count, body, 0)

    return product


def scatter_scratch(rows, hidden, dtype):
    dma = pltpu.SemaphoreType.DMA
    return [pltpu.VMEM((4, 2 * rows, hidden), dtype), pltpu.VMEM((4, rows, hidden), dtype),
            pltpu.VMEM((2, rows // 2, hidden), dtype), pltpu.VMEM((2, rows, hidden), dtype), dma((10,)), dma((10,))]


def scatter_norm_kernel(n, tile, x_ref, w_ref, res_ref, gain_ref, mid_ref, norm_ref,
                        x_s, w_s, lhs, res_s, part, pin, mid, fin, send, recv, load, wl):
    ring = Ring(n)
    loads = [pltpu.make_async_copy(a, b, load.at[i]) for i, (a, b) in enumerate(((x_ref, x_s), (res_ref, res_s)))]
    weights = Weights(w_ref, w_s, wl, tile, False)
    loads[0].start()
    weights.start()
    loads[1].start()
    ring.barrier()
    loads[0].wait()
    sc = Scatter(ring, part, pin, mid, fin, send, recv)

    def emit(at, total):
        x1 = (res_s[at, :].astype(jnp.float32) + total.astype(jnp.float32)).astype(jnp.bfloat16)
        mid_ref[at, :] = x1
        norm_ref[at, :] = (normalized(x1.astype(jnp.float32))[0] * gain_ref[...]).astype(jnp.bfloat16)

    sc.run(product_t(ring, tile, x_s, weights, lhs, part), lambda: loads[1].wait(), emit)


def scatter_norm(n, cid, x, w, res, gain, tile=512):
    (m, seq), hidden = x.shape, w.shape[1]
    rows = seq // n
    dma = pltpu.SemaphoreType.DMA
    vmem = lambda *d: pltpu.VMEM(d, x.dtype)
    any_spec, vm = pl.BlockSpec(memory_space=pl.ANY), pl.BlockSpec(memory_space=pltpu.VMEM)
    return pl.pallas_call(
        functools.partial(scatter_norm_kernel, n, tile),
        in_specs=[any_spec] * 3 + [vm],
        out_specs=[vm] * 2,
        out_shape=[jax.ShapeDtypeStruct((rows, hidden), x.dtype)] * 2,
        scratch_shapes=[vmem(*x.shape), vmem(*w.shape), vmem(2 * rows, m), vmem(rows, hidden)]
        + scatter_scratch(rows, hidden, x.dtype) + [dma((2,)), dma((hidden // tile,))],
        compiler_params=pltpu.CompilerParams(collective_id=cid, has_side_effects=True, vmem_limit_bytes=60 * 2 ** 20),
        cost_estimate=pl.CostEstimate(flops=40 * 10 ** 9, bytes_accessed=3 * seq * hidden, transcendentals=0),
        name="scatter_norm",
    )(x, w, res, gain)


def scatter_grads_kernel(n, tile, x_ref, w_ref, a_ref, o_ref, d_ref, res_ref, dmid_ref, gain_ref, dg2_ref,
                         out_ref, gq_ref, go_ref, sums_ref,
                         x_s, w_s, lhs, o_s, a_s, d_s, gq_st, go_st, res_s, dmid_s, acc, mine, slots,
                         part, pin, mid, fin, send, recv, load, wl, a_l, a_p, d_l, d_p, gsend, grecv):
    ring = Ring(n)
    peers = [lax.rem(ring.me + k, n) for k in range(1, n)]
    loads = [pltpu.make_async_copy(a, b, load.at[i]) for i, (a, b) in
             enumerate(((x_ref, x_s), (o_ref, o_s), (res_ref, res_s), (dmid_ref, dmid_s)))]
    weights = Weights(w_ref, w_s, wl, tile, False)
    loads[0].start()
    weights.start()
    wq = Product(a_ref, x_s, gq_ref, a_s, gq_st, a_l, a_p, False)
    wo = Product(d_ref, o_s, go_ref, d_s, go_st, d_l, d_p, False)
    ring.barrier(peers)
    for cp in loads[1:]:
        cp.start()
    wq.get(0).start()
    wo.get(0).start()
    loads[0].wait()
    sc = Scatter(ring, part, pin, mid, fin, send, recv)
    acc[...] = jnp.zeros_like(acc)

    def filler():
        loads[1].wait()
        wq.run(0, wq.total)
        wo.run(0, wo.total)
        loads[2].wait()
        loads[3].wait()

    def emit(at, total):
        hat, _ = normalized(res_s[at, :].astype(jnp.float32))
        out_ref[at, :] = total
        acc[...] += fold_rows(total.astype(jnp.float32) * hat)

    sc.run(product_t(ring, tile, x_s, weights, lhs, part), filler, emit)
    mine[0:1, :] = jnp.sum(acc[...], axis=0, keepdims=True)
    mine[1:2, :] = dg2_ref[...]
    step = 16

    def body(i, c):
        at = rows_at(i * step, step)
        hat, rstd = normalized(res_s[at, :].astype(jnp.float32))
        dx = norm_backward(hat, rstd, gain_ref[...], out_ref[at, :].astype(jnp.float32))
        out_ref[at, :] = (dmid_s[at, :].astype(jnp.float32) + dx).astype(jnp.bfloat16)
        return c

    steps = out_ref.shape[0] // step
    lax.fori_loop(0, steps // 4, body, 0)
    copies = [pltpu.make_async_remote_copy(src_ref=mine, dst_ref=slots.at[ring.me], send_sem=gsend.at[k], recv_sem=grecv.at[k],
                                           device_id={'model': dev}, device_id_type=MESH) for k, dev in enumerate(peers)]
    for cp in copies:
        cp.start()
    slots[ring.me] = mine[...]
    lax.fori_loop(steps // 4, steps, body, 0)
    wq.finish()
    wo.finish()
    for cp in copies:
        cp.wait()
    total = slots[0]
    for k in range(1, n):
        total = total + slots[k]
    sums_ref[...] = total.astype(jnp.bfloat16)


def scatter_grads(n, cid, x, w, a, o, d, res, d_mid, gain, dg2, tile=512):
    (m, seq), hidden = x.shape, w.shape[1]
    rows = seq // n
    dma = pltpu.SemaphoreType.DMA
    vmem = lambda *s: pltpu.VMEM(s, x.dtype)
    any_spec, vm = pl.BlockSpec(memory_space=pl.ANY), pl.BlockSpec(memory_space=pltpu.VMEM)
    return pl.pallas_call(
        functools.partial(scatter_grads_kernel, n, tile),
        in_specs=[any_spec] * 7 + [vm] * 2,
        out_specs=[vm, any_spec, any_spec, vm],
        out_shape=[jax.ShapeDtypeStruct((rows, hidden), x.dtype), jax.ShapeDtypeStruct(w.shape, x.dtype),
                   jax.ShapeDtypeStruct((o.shape[0], hidden), x.dtype), jax.ShapeDtypeStruct((2, hidden), x.dtype)],
        scratch_shapes=[vmem(*x.shape), vmem(*w.shape), vmem(2 * rows, m), vmem(*o.shape), vmem(2, seq, tile), vmem(2, seq, tile),
                        vmem(2, m, tile), vmem(2, o.shape[0], tile), vmem(rows, hidden), vmem(rows, hidden),
                        pltpu.VMEM((8, hidden), jnp.float32), pltpu.VMEM((2, hidden), jnp.float32),
                        pltpu.VMEM((n, 2, hidden), jnp.float32)]
        + scatter_scratch(rows, hidden, x.dtype)
        + [dma((4,)), dma((hidden // tile,)), dma((2,)), dma((2,)), dma((2,)), dma((2,)), dma((n - 1,)), dma((n - 1,))],
        compiler_params=pltpu.CompilerParams(collective_id=cid, has_side_effects=True, vmem_limit_bytes=63 * 2 ** 20),
        cost_estimate=pl.CostEstimate(flops=60 * 10 ** 9, bytes_accessed=6 * seq * hidden, transcendentals=0),
        name="scatter_grads",
    )(x, w, a, o, d, res, d_mid, gain, dg2)


def scatter_mlp_kernel(n, tile, dz_ref, up_ref, g_ref, down_ref, res_ref, dy_ref, gain_ref, out_ref, y_ref, dg_ref,
                       dz_s, w_s, g_s, down_s, res_s, dy_s, acc, part, pin, mid, fin, send, recv, load, wl, zl, ystage, put):
    ring = Ring(n)
    loads = [pltpu.make_async_copy(a, b, load.at[i]) for i, (a, b) in
             enumerate(((res_ref, res_s), (dy_ref, dy_s), (g_ref, g_s), (down_ref, down_s)))]
    wide = part.shape[1]
    hidden = part.shape[2]

    def dz_at(d):
        return rows_at(ring.ahead(d) * wide, wide)

    dz_loads = [pltpu.make_async_copy(dz_ref.at[dz_at(d)], dz_s.at[dz_at(d)], zl.at[d]) for d in range(4)]
    weights = Weights(up_ref, w_s, wl, tile, True)
    dz_loads[2].start()
    weights.start()
    ring.barrier()
    for d in (1, 3, 0):
        dz_loads[d].start()
    sc = Scatter(ring, part, pin, mid, fin, send, recv)
    acc[...] = jnp.zeros_like(acc)

    def product(d, row0, count, first):
        if first or d != 2:
            dz_loads[d].wait()
        if d == 3:
            for cp in loads:
                cp.start()
        src = rows_at(ring.ahead(d) * wide + row0, count, 256)
        at = rows_at(row0, count, 256)

        def body(t, c):
            cols = rows_at(t * tile, tile)
            if first:
                weights.copy(t).wait()
            part[d, at, cols] = dot_nt(dz_s[src, :], w_s[cols, :]).astype(jnp.bfloat16)
            return c

        lax.fori_loop(0, hidden // tile, body, 0)

    def emit(at, total):
        d = total.astype(jnp.float32)
        hat, rstd = normalized(res_s[at, :].astype(jnp.float32))
        dx = norm_backward(hat, rstd, gain_ref[...], d)
        out_ref[at, :] = (dy_s[at, :].astype(jnp.float32) + dx).astype(jnp.bfloat16)
        acc[...] += fold_rows(d * hat)

    def filler():
        for cp in loads:
            cp.wait()
        puts = []
        for q in range(n // 2):
            if q >= 2:
                puts[q - 2].wait()

            def body(t, c):
                cols = rows_at(t * tile, tile)
                ystage[q % 2, :, cols] = dot32(g_s[q * wide:(q + 1) * wide, :], down_s[:, cols]).astype(jnp.bfloat16)
                return c

            lax.fori_loop(0, hidden // tile, body, 0)
            puts.append(pltpu.make_async_copy(ystage.at[q % 2], y_ref.at[q * wide:(q + 1) * wide], put.at[q]))
            puts[q].start()
        for cp in puts[-2:]:
            cp.wait()

    sc.run(product, filler, emit)
    dg_ref[...] = jnp.sum(acc[...], axis=0, keepdims=True)


def scatter_mlp(n, cid, dz, up, g, down, res, dy, gain, tile=512):
    (seq, ffn), hidden = dz.shape, down.shape[1]
    rows = seq // n
    dma = pltpu.SemaphoreType.DMA
    any_spec, vm = pl.BlockSpec(memory_space=pl.ANY), pl.BlockSpec(memory_space=pltpu.VMEM)
    return pl.pallas_call(
        functools.partial(scatter_mlp_kernel, n, tile),
        in_specs=[any_spec] * 6 + [vm],
        out_specs=[vm, any_spec, vm],
        out_shape=[jax.ShapeDtypeStruct((rows, hidden), dz.dtype), jax.ShapeDtypeStruct((seq, hidden), dz.dtype),
                   jax.ShapeDtypeStruct((1, hidden), jnp.float32)],
        scratch_shapes=[pltpu.VMEM(a.shape, a.dtype) for a in (dz, up, g, down, res, dy)]
        + [pltpu.VMEM((8, hidden), jnp.float32)] + scatter_scratch(rows, hidden, dz.dtype)
        + [dma((4,)), dma((hidden // tile,)), dma((4,)), pltpu.VMEM((2, 2 * rows, hidden), dz.dtype), dma((n // 2,))],
        compiler_params=pltpu.CompilerParams(collective_id=cid, has_side_effects=True, vmem_limit_bytes=63 * 2 ** 20),
        cost_estimate=pl.CostEstimate(flops=60 * 10 ** 9, bytes_accessed=3 * seq * hidden, transcendentals=0),
        name="scatter_mlp",
    )(dz, up, g, down, res, dy, gain)


def local_layer(n, hidden_in, seg_ids, gain_attn, w_qkv, w_out, gain_mlp, w_up, w_down, grad_out):
    heads, hd, hidden = w_out.shape
    seq_len = seg_ids.shape[1]
    x_f32 = hidden_in[0].astype(jnp.float32)
    dy = grad_out[0]
    wq_t = jnp.transpose(w_qkv, (1, 2, 3, 0)).reshape(heads * 3 * hd, hidden)
    wo = w_out.reshape(heads * hd, hidden)
    first = jnp.sum(seg_ids[0][:, None] < seg_ids[0][None, :], axis=0, dtype=jnp.int32)
    lo = first[::BLK] // BLK
    first = first[None]
    gather = lambda a: lax.all_gather(a, 'model', axis=0, tiled=True)
    scatter = lambda a: lax.psum_scatter(a, 'model', scatter_dimension=0, tiled=True)

    gain1 = gain_attn.astype(jnp.float32)
    gain2 = gain_mlp.astype(jnp.float32)[None]
    attn_in, qkv_t = gather_t(n, 0, layer_norm(x_f32, gain1).astype(jnp.bfloat16), wq_t, 320)
    dy_late, qkv_t = lax.optimization_barrier((dy, qkv_t))
    grad_full = gather(dy_late)
    o_t, lse = attention_fwd(qkv_t, lo, first, heads, hd)
    mid_loc, norm2 = scatter_norm(n, 1, o_t, wo, hidden_in[0], gain2)
    mlp_in, act_lo, d_pre = mlp(n, 2, norm2, grad_full, w_up, w_down)
    d_mid, mlp_part, d_gain_mlp = scatter_mlp(n, 3, d_pre, w_up, act_lo, w_down, mid_loc, dy, gain2)
    d_mid_full, do_t, g_up, g_down = gather_grads(n, 4, d_mid, wo, mlp_in, d_pre, act_lo, grad_full)
    mlp_part, do_t = lax.optimization_barrier((mlp_part, do_t))
    mlp_sum = scatter(mlp_part)
    hidden_out = (mid_loc.astype(jnp.float32) + mlp_sum.astype(jnp.float32)).astype(jnp.bfloat16)
    dqkv_t, g_up, g_down = attention_bwd(qkv_t, o_t, do_t, lse, lo, first, g_up, g_down, heads, hd)
    grad_in, g_qkv, g_out, gain_sums = scatter_grads(n, 5, dqkv_t, wq_t, attn_in, o_t, d_mid_full, hidden_in[0], d_mid,
                                                     gain1[None], d_gain_mlp)
    g_qkv = jnp.transpose(g_qkv.reshape(heads, 3, hd, hidden), (3, 0, 1, 2))
    return (hidden_out[None], grad_in[None], g_qkv, g_out.reshape(heads, hd, hidden), g_up, g_down,
            gain_sums[0], gain_sums[1])


def solution(mesh):
    act_spec = P('data', 'model', None)
    in_specs = (act_spec, P('data', None), P(), P(None, 'model', None, None), P('model', None, None), P(), P(None, 'model'), P('model', None), act_spec)
    out_specs = (act_spec, act_spec, P('data', 'model', None, None), P(('data', 'model'), None, None), P('data', 'model'), P(('data', 'model'), None), P('data'), P('data'))
    return jax.shard_map(functools.partial(local_layer, mesh.shape['model']), mesh=mesh, in_specs=in_specs, out_specs=out_specs, check_vma=False)
```

```python
import functools

import jax
import jax.numpy as jnp
from jax import lax
from jax.experimental import pallas as pl
from jax.experimental.pallas import tpu as pltpu
from jax.sharding import PartitionSpec as P

LN_EPS = 1e-5
BLK = 256
NT = (((1,), (1,)), ((), ()))
MESH = pl.DeviceIdType.MESH


def layer_norm(x_f32, gain_f32):
    mean_val = jnp.mean(x_f32, axis=-1, keepdims=True)
    centered = x_f32 - mean_val
    variance = jnp.mean(centered * centered, axis=-1, keepdims=True)
    return centered * lax.rsqrt(variance + LN_EPS) * gain_f32


def gelu_tanh(pre_act):
    return jax.nn.gelu(pre_act, approximate=True)


def dot32(a, b):
    return jnp.dot(a, b, preferred_element_type=jnp.float32)


def visible(j, i, first_row):
    kpos = j * BLK + lax.broadcasted_iota(jnp.int32, (BLK, BLK), 0)
    qpos = i * BLK + lax.broadcasted_iota(jnp.int32, (BLK, BLK), 1)
    return (kpos <= qpos) & (kpos >= first_row)


def attn_fwd_kernel(heads, hd, lo_ref, qkv_ref, first_ref, o_ref, lse_ref, k_s, s_s, o_s):
    i = pl.program_id(0)
    scale = hd ** -0.5

    @pl.when(i == 0)
    def _():
        for h in range(heads):
            for j in range(k_s.shape[1] // BLK):
                kt = qkv_ref[(3 * h + 1) * hd:(3 * h + 2) * hd, j * BLK:(j + 1) * BLK]
                k_s[h, j * BLK:(j + 1) * BLK, :] = kt.T

    lo = lo_ref[i]
    cols = pl.ds(pl.multiple_of(i * BLK, BLK), BLK)
    first_row = first_ref[0:1, cols]
    neg = jnp.full((8, BLK), -jnp.inf, jnp.float32)

    def scores(j, m):
        rows = pl.ds(pl.multiple_of(j * BLK, BLK), BLK)
        mask = visible(j, i, first_row)
        out = []
        for h in range(heads):
            s = dot32(k_s[h, rows, :], qkv_ref[3 * h * hd:(3 * h + 1) * hd, cols]) * scale
            s = jnp.where(mask, s, -1e30)
            s_s[h, rows, :] = s
            out.append(jnp.maximum(m[h], jnp.max(s.reshape(BLK // 8, 8, BLK), axis=0)))
        return tuple(out)

    m = lax.fori_loop(lo, i + 1, scores, (neg,) * heads)
    m = [jnp.max(x, axis=0, keepdims=True) for x in m]

    def expo(j, l):
        rows = pl.ds(pl.multiple_of(j * BLK, BLK), BLK)
        out = []
        for h in range(heads):
            e = jnp.exp(s_s[h, rows, :] - m[h])
            s_s[h, rows, :] = e
            out.append(l[h] + jnp.sum(e.reshape(BLK // 8, 8, BLK), axis=0))
        return tuple(out)

    l = lax.fori_loop(lo, i + 1, expo, (jnp.zeros((8, BLK), jnp.float32),) * heads)
    l = [jnp.sum(x, axis=0, keepdims=True) for x in l]
    r = [1.0 / x for x in l]
    for h in range(heads):
        lse_ref[h:h + 1, :] = m[h] + jnp.log(l[h])
        o_s[h] = jnp.zeros((hd, BLK), jnp.float32)

    def values(j, c):
        rows = pl.ds(pl.multiple_of(j * BLK, BLK), BLK)
        for h in range(heads):
            pb = (s_s[h, rows, :] * r[h]).astype(jnp.bfloat16)
            o_s[h] += dot32(qkv_ref[(3 * h + 2) * hd:(3 * h + 3) * hd, rows], pb)
        return c

    lax.fori_loop(lo, i + 1, values, 0)
    for h in range(heads):
        o_ref[h * hd:(h + 1) * hd, :] = o_s[h].astype(jnp.bfloat16)


def attention_fwd(qkv_t, lo, first, heads, hd):
    seq = qkv_t.shape[1]
    nb = seq // BLK
    flops = 4 * heads * seq * seq * hd // 2
    return pl.pallas_call(
        functools.partial(attn_fwd_kernel, heads, hd),
        grid_spec=pltpu.PrefetchScalarGridSpec(
            num_scalar_prefetch=1, grid=(nb,),
            in_specs=[pl.BlockSpec(qkv_t.shape, lambda i, lo: (0, 0)),
                      pl.BlockSpec((1, seq), lambda i, lo: (0, 0))],
            out_specs=[pl.BlockSpec((heads * hd, BLK), lambda i, lo: (0, i)),
                       pl.BlockSpec((8, BLK), lambda i, lo: (0, i))],
            scratch_shapes=[pltpu.VMEM((heads, seq, hd), jnp.bfloat16),
                            pltpu.VMEM((heads, seq, BLK), jnp.float32),
                            pltpu.VMEM((heads, hd, BLK), jnp.float32)]),
        out_shape=[jax.ShapeDtypeStruct((heads * hd, seq), jnp.bfloat16),
                   jax.ShapeDtypeStruct((8, seq), jnp.float32)],
        compiler_params=pltpu.CompilerParams(vmem_limit_bytes=56 * 2 ** 20),
        cost_estimate=pl.CostEstimate(flops=8 * flops, bytes_accessed=2 * qkv_t.size, transcendentals=0),
        name="attn_fwd",
    )(lo, qkv_t, first)


def attn_bwd_kernel(heads, hd, lo_ref, qkv_ref, o_ref, do_ref, lse_ref, first_ref, up_ref, down_ref, d_ref, up_out, down_out,
                    k_s, v_s, dq_s, dk_s, dv_s):
    i = pl.program_id(0)
    seq = qkv_ref.shape[1]
    scale = hd ** -0.5

    @pl.when(i == 0)
    def _():
        dk_s[...] = jnp.zeros_like(dk_s)
        dv_s[...] = jnp.zeros_like(dv_s)
        for h in range(heads):
            for j in range(seq // BLK):
                c = slice(j * BLK, (j + 1) * BLK)
                k_s[h, c, :] = qkv_ref[(3 * h + 1) * hd:(3 * h + 2) * hd, c].T
                v_s[h, c, :] = qkv_ref[(3 * h + 2) * hd:(3 * h + 3) * hd, c].T

    up_out[...] = up_ref[...]
    down_out[...] = down_ref[...]
    lo = lo_ref[i]
    cols = pl.ds(pl.multiple_of(i * BLK, BLK), BLK)
    first_row = first_ref[0:1, cols]
    delta = []
    for h in range(heads):
        hs = slice(h * hd, (h + 1) * hd)
        delta.append(jnp.sum(do_ref[hs, :].astype(jnp.float32) * o_ref[hs, :].astype(jnp.float32), axis=0, keepdims=True))
        dq_s[h] = jnp.zeros((hd, BLK), jnp.float32)

    def step(j, c):
        rows = pl.ds(pl.multiple_of(j * BLK, BLK), BLK)
        mask = visible(j, i, first_row)
        for h in range(heads):
            q_t = qkv_ref[3 * h * hd:(3 * h + 1) * hd, cols]
            do_t = do_ref[h * hd:(h + 1) * hd, :]
            s = dot32(k_s[h, rows, :], q_t) * scale
            p = jnp.exp(jnp.where(mask, s, -1e30) - lse_ref[h:h + 1, :])
            dp = dot32(v_s[h, rows, :], do_t)
            ds = (p * (dp - delta[h]) * scale).astype(jnp.bfloat16)
            pb = p.astype(jnp.bfloat16)
            dq_s[h] += dot32(qkv_ref[(3 * h + 1) * hd:(3 * h + 2) * hd, rows], ds)
            dk_s[h, :, rows] += lax.dot_general(q_t, ds, NT, preferred_element_type=jnp.float32)
            dv_s[h, :, rows] += lax.dot_general(do_t, pb, NT, preferred_element_type=jnp.float32)
        return c

    lax.fori_loop(lo, i + 1, step, 0)
    for h in range(heads):
        d_ref[3 * h * hd:(3 * h + 1) * hd, cols] = dq_s[h].astype(jnp.bfloat16)

    @pl.when(i == pl.num_programs(0) - 1)
    def _():
        for h in range(heads):
            d_ref[(3 * h + 1) * hd:(3 * h + 2) * hd, :] = dk_s[h].astype(jnp.bfloat16)
            d_ref[(3 * h + 2) * hd:(3 * h + 3) * hd, :] = dv_s[h].astype(jnp.bfloat16)


def attention_bwd(qkv_t, o_t, do_t, lse, lo, first, g_up, g_down, heads, hd):
    seq = qkv_t.shape[1]
    nb = seq // BLK
    flops = 10 * heads * seq * seq * hd // 2
    blk = lambda rows: pl.BlockSpec((rows, BLK), lambda i, lo: (0, i))
    through = [pl.BlockSpec((a.shape[0] // nb, a.shape[1]), lambda i, lo: (i, 0)) for a in (g_up, g_down)]
    return pl.pallas_call(
        functools.partial(attn_bwd_kernel, heads, hd),
        grid_spec=pltpu.PrefetchScalarGridSpec(
            num_scalar_prefetch=1, grid=(nb,),
            in_specs=[pl.BlockSpec(qkv_t.shape, lambda i, lo: (0, 0)), blk(heads * hd), blk(heads * hd), blk(8),
                      pl.BlockSpec((1, seq), lambda i, lo: (0, 0))] + through,
            out_specs=[pl.BlockSpec(qkv_t.shape, lambda i, lo: (0, 0))] + through,
            scratch_shapes=[pltpu.VMEM((heads, seq, hd), jnp.bfloat16),
                            pltpu.VMEM((heads, seq, hd), jnp.bfloat16),
                            pltpu.VMEM((heads, hd, BLK), jnp.float32),
                            pltpu.VMEM((heads, hd, seq), jnp.float32),
                            pltpu.VMEM((heads, hd, seq), jnp.float32)]),
        out_shape=[jax.ShapeDtypeStruct(a.shape, jnp.bfloat16) for a in (qkv_t, g_up, g_down)],
        compiler_params=pltpu.CompilerParams(vmem_limit_bytes=56 * 2 ** 20),
        cost_estimate=pl.CostEstimate(flops=8 * flops, bytes_accessed=4 * qkv_t.size, transcendentals=0),
        name="attn_bwd",
    )(lo, qkv_t, o_t, do_t, lse, first, g_up, g_down)


def dot_nt(a, b):
    return lax.dot_general(a, b, NT, preferred_element_type=jnp.float32)


class Ring:
    def __init__(self, n):
        self.n = n
        self.me = lax.axis_index('model')
        self.core = lax.rem(self.me, 2)
        self.chip = self.me // 2
        self.partner = self.me + 1 - 2 * self.core
        self.next = lax.rem(self.me + 2, n)
        self.prev = lax.rem(self.me + n - 2, n)
        self.opp = lax.rem(self.me + n // 2, n)

    def barrier(self, peers=None):
        sem = pltpu.get_barrier_semaphore()
        peers = peers or (self.partner, self.next, self.prev)
        for dev in peers:
            pl.semaphore_signal(sem, inc=1, device_id={'model': dev}, device_id_type=MESH)
        pl.semaphore_wait(sem, len(peers))

    def ahead(self, d):
        return lax.rem(self.chip + d, self.n // 2)


def rows_at(start, size, unit=None):
    return pl.ds(pl.multiple_of(start, unit or size), size)


class Gather:
    def __init__(self, ring, buf, send, recv):
        self.ring, self.buf, self.send, self.recv = ring, buf, send, recv
        self.rows = buf.shape[0] // ring.n
        self.half = self.rows // 2
        r = ring
        self.table = {0: (r.me, None, r.partner),
                      1: (r.me, 0, r.next), 2: (r.me, 1, r.next), 3: (r.prev, 0, r.next),
                      4: (r.me, 1, r.prev), 5: (r.me, 0, r.prev), 6: (r.next, 1, r.prev),
                      7: (r.prev, 0, r.partner), 8: (r.prev, 1, r.partner),
                      9: (r.next, 1, r.partner), 10: (r.next, 0, r.partner),
                      11: (r.opp, 0, r.partner), 12: (r.opp, 1, r.partner)}

    def copy(self, k):
        owner, part, dev = self.table[k]
        if part is None:
            ref = self.buf.at[rows_at(owner * self.rows, self.rows)]
        else:
            ref = self.buf.at[rows_at(owner * self.rows + part * self.half, self.half)]
        return pltpu.make_async_remote_copy(src_ref=ref, dst_ref=ref, send_sem=self.send.at[k], recv_sem=self.recv.at[k],
                                            device_id={'model': dev}, device_id_type=MESH)

    def start(self, *ks):
        for k in ks:
            self.copy(k).start()

    def arrived(self, *ks):
        for k in ks:
            self.copy(k).wait_recv()

    def run(self, compute, fill=lambda k: None):
        self.start(1, 4, 0, 2, 5)
        self.arrived(0)
        compute(self.ring.chip)
        fill(0)
        self.arrived(1)
        self.start(3, 7)
        self.arrived(4)
        self.start(6, 9)
        fill(1)
        self.arrived(2)
        self.start(8)
        self.arrived(5)
        self.start(10)
        self.arrived(7, 8)
        compute(self.ring.ahead(self.ring.n // 2 - 1))
        self.arrived(9, 10)
        compute(self.ring.ahead(1))
        fill(2)
        self.arrived(3)
        self.start(11)
        self.arrived(6)
        self.start(12)
        self.arrived(11, 12)
        compute(self.ring.ahead(self.ring.n // 4))
        for k in self.table:
            self.copy(k).wait_send()


def gather_t_kernel(n, tile, x_ref, w_ref, full_ref, out_ref, buf, w_s, stage, send, recv, load, store, put):
    ring = Ring(n)
    rows = x_ref.shape[0]
    mine = pltpu.make_async_copy(x_ref, buf.at[rows_at(ring.me * rows, rows)], load.at[0])
    mine.start()
    weights = pltpu.make_async_copy(w_ref, w_s, load.at[1])
    weights.start()
    ring.barrier()
    mine.wait()
    g = Gather(ring, buf, send, recv)
    pending = []

    def compute(chip):
        s = len(pending)
        if s == 0:
            weights.wait()
        at = rows_at(chip * (2 * rows), 2 * rows)
        keep = pltpu.make_async_copy(buf.at[at], full_ref.at[at], store.at[s])
        keep.start()

        def body(t, c):
            w_rows = rows_at(t * tile, tile)
            stage[s, w_rows, :] = dot_nt(w_s[w_rows, :], buf[at, :]).astype(jnp.bfloat16)
            return c

        lax.fori_loop(0, w_s.shape[0] // tile, body, 0)
        out = pltpu.make_async_copy(stage.at[s], out_ref.at[:, at], put.at[s])
        out.start()
        pending.append((keep, out))

    g.run(compute)
    for pair in pending:
        for cp in pair:
            cp.wait()


def gather_t(n, cid, x, w, tile):
    rows, hidden = x.shape
    seq, m, chips = rows * n, w.shape[0], n // 2
    dma = pltpu.SemaphoreType.DMA
    return pl.pallas_call(
        functools.partial(gather_t_kernel, n, tile),
        in_specs=[pl.BlockSpec(memory_space=pl.ANY)] * 2,
        out_specs=[pl.BlockSpec(memory_space=pl.ANY)] * 2,
        out_shape=[jax.ShapeDtypeStruct((seq, hidden), x.dtype), jax.ShapeDtypeStruct((m, seq), x.dtype)],
        scratch_shapes=[pltpu.VMEM((seq, hidden), x.dtype), pltpu.VMEM(w.shape, w.dtype),
                        pltpu.VMEM((chips, m, 2 * rows), x.dtype),
                        dma((13,)), dma((13,)), dma((2,)), dma((chips,)), dma((chips,))],
        compiler_params=pltpu.CompilerParams(collective_id=cid, has_side_effects=True, vmem_limit_bytes=60 * 2 ** 20),
        cost_estimate=pl.CostEstimate(flops=40 * 10 ** 9, bytes_accessed=3 * seq * hidden, transcendentals=0),
        name="gather_t",
    )(x, w)


def mlp_kernel(n, tile, x_ref, dy_ref, up_ref, down_ref, full_ref, g_ref, dz_ref,
               buf, dy_s, up_s, down_s, g_s, dz_s, da_s, send, recv, load, store, put, put2, dy_sem):
    ring = Ring(n)
    rows = x_ref.shape[0]
    mine = pltpu.make_async_copy(x_ref, buf.at[rows_at(ring.me * rows, rows)], load.at[0])
    mine.start()
    w_up = pltpu.make_async_copy(up_ref, up_s, load.at[1])
    w_up.start()
    w_down = pltpu.make_async_copy(down_ref, down_s, load.at[2])
    w_down.start()
    order = [ring.chip, ring.ahead(n // 2 - 1), ring.ahead(1), ring.ahead(n // 4)]

    def dy_copy(s):
        return pltpu.make_async_copy(dy_ref.at[rows_at(order[s] * (2 * rows), 2 * rows)], dy_s.at[s % 2], dy_sem.at[s])

    dy_copy(0).start()
    dy_copy(1).start()
    ring.barrier()
    mine.wait()
    g = Gather(ring, buf, send, recv)
    pending = []
    root = (2.0 / jnp.pi) ** 0.5

    def compute(chip):
        s = len(pending)
        if s == 0:
            w_up.wait()
            w_down.wait()
        at = rows_at(chip * (2 * rows), 2 * rows)
        keep = pltpu.make_async_copy(buf.at[at], full_ref.at[at], store.at[s])
        keep.start()
        if s >= 2:
            for cp in pending[s - 2][1:]:
                cp.wait()
        if s == 0:
            dy_copy(0).wait()

        def body(t, c):
            cols = rows_at(t * tile, tile)
            z = dot32(buf[at, :], up_s[:, cols])
            if s == 0:
                da = dot_nt(dy_s[0], down_s[cols, :])
            else:
                da = da_s[s - 1, :, cols]
            z2 = z * z
            th = jnp.tanh(root * (z + 0.044715 * (z2 * z)))
            cdf = 0.5 * (1.0 + th)
            g_s[s % 2, :, cols] = (z * cdf).astype(jnp.bfloat16)
            slope = cdf + (0.5 * z) * (1.0 - th * th) * (root * (1.0 + (3 * 0.044715) * z2))
            dz_s[s % 2, :, cols] = (slope * da).astype(jnp.bfloat16)
            return c

        lax.fori_loop(0, up_s.shape[1] // tile, body, 0)
        if s == 0:
            dy_copy(2).start()
        og = pltpu.make_async_copy(g_s.at[s % 2], g_ref.at[at], put.at[s])
        od = pltpu.make_async_copy(dz_s.at[s % 2], dz_ref.at[at], put2.at[s])
        og.start()
        od.start()
        pending.append((keep, og, od))

    def fill(k):
        if k == 1:
            for s in range(1, n // 2):
                dy_copy(s).wait()

                def body(t, c):
                    cols = rows_at(t * tile, tile)
                    da_s[s - 1, :, cols] = dot_nt(dy_s[s % 2], down_s[cols, :])
                    return c

                lax.fori_loop(0, up_s.shape[1] // tile, body, 0)
                if s + 2 < n // 2:
                    dy_copy(s + 2).start()

    g.run(compute, fill)
    for s, cps in enumerate(pending):
        for cp in (cps if s >= n // 2 - 2 else cps[:1]):
            cp.wait()


def mlp(n, cid, x, dy, up, down, tile=256):
    rows, hidden = x.shape
    seq, ffn, chips = rows * n, up.shape[1], n // 2
    dma = pltpu.SemaphoreType.DMA
    return pl.pallas_call(
        functools.partial(mlp_kernel, n, tile),
        in_specs=[pl.BlockSpec(memory_space=pl.ANY)] * 4,
        out_specs=[pl.BlockSpec(memory_space=pl.ANY)] * 3,
        out_shape=[jax.ShapeDtypeStruct((seq, hidden), x.dtype)] + [jax.ShapeDtypeStruct((seq, ffn), x.dtype)] * 2,
        scratch_shapes=[pltpu.VMEM((seq, hidden), x.dtype), pltpu.VMEM((2, 2 * rows, hidden), x.dtype),
                        pltpu.VMEM(up.shape, x.dtype), pltpu.VMEM(down.shape, x.dtype),
                        pltpu.VMEM((2, 2 * rows, ffn), x.dtype), pltpu.VMEM((2, 2 * rows, ffn), x.dtype),
                        pltpu.VMEM((chips - 1, 2 * rows, ffn), jnp.float32),
                        dma((13,)), dma((13,)), dma((3,)), dma((chips,)), dma((chips,)), dma((chips,)), dma((chips,))],
        compiler_params=pltpu.CompilerParams(collective_id=cid, has_side_effects=True, vmem_limit_bytes=60 * 2 ** 20),
        cost_estimate=pl.CostEstimate(flops=40 * 10 ** 9, bytes_accessed=3 * seq * hidden, transcendentals=0),
        name="gather_mlp",
    )(x, dy, up, down)


class Product:
    def __init__(self, x, fixed, out, slots, stage, load, store, rows, lhs=None):
        self.x, self.fixed, self.out, self.slots, self.stage = x, fixed, out, slots, stage
        self.load, self.store, self.rows, self.lhs = load, store, rows, lhs
        self.unit = slots.shape[2]
        self.total = x.shape[1] // self.unit

    def get(self, u):
        slot = lax.rem(u, 2)
        return pltpu.make_async_copy(self.x.at[:, rows_at(u * self.unit, self.unit)], self.slots.at[slot], self.load.at[slot])

    def put(self, u):
        slot = lax.rem(u, 2)
        at = rows_at(u * self.unit, self.unit)
        dst = self.out.at[at] if self.rows else self.out.at[:, at]
        return pltpu.make_async_copy(self.stage.at[slot], dst, self.store.at[slot])

    def run(self, first, last):
        def body(u, c):
            slot = lax.rem(u, 2)
            self.get(u).wait()

            @pl.when(u + 1 < self.total)
            def _():
                self.get(u + 1).start()

            @pl.when(u >= 2)
            def _():
                self.put(u - 2).wait()

            if self.rows:
                self.lhs[...] = self.slots[slot].T
                width = self.fixed.shape[1]
                for w in range(0, width, 1280):
                    at = slice(w, min(w + 1280, width))
                    self.stage[slot, :, at] = dot32(self.lhs[...], self.fixed[:, at]).astype(jnp.bfloat16)
            else:
                step = 320

                def part(t, c):
                    at = rows_at(t * step, step)
                    self.stage[slot, at, :] = dot32(self.fixed[at, :], self.slots[slot]).astype(jnp.bfloat16)
                    return c

                lax.fori_loop(0, self.fixed.shape[0] // step, part, 0)
            self.put(u).start()
            return c

        lax.fori_loop(first, last, body, 0)

    def finish(self):
        self.put(self.total - 2).wait()
        self.put(self.total - 1).wait()


def gather_grads_kernel(n, x_ref, w_ref, b_ref, dz_ref, g_ref, dy_ref, full_ref, out_ref, up_ref, down_ref,
                        buf, w_s, stage, dz_s, dy_s, b_s, g_s, lhs, up_st, down_st,
                        send, recv, load, store, put, up_l, up_p, down_l, down_p):
    ring = Ring(n)
    rows = x_ref.shape[0]
    loads = [pltpu.make_async_copy(a, b, load.at[i]) for i, (a, b) in
             enumerate(((x_ref, buf.at[rows_at(ring.me * rows, rows)]), (w_ref, w_s), (dz_ref, dz_s), (dy_ref, dy_s)))]
    up = Product(b_ref, dz_s, up_ref, b_s, up_st, up_l, up_p, True, lhs)
    down = Product(g_ref, dy_s, down_ref, g_s, down_st, down_l, down_p, True, lhs)
    loads[0].start()
    loads[1].start()
    up.get(0).start()
    loads[2].start()
    down.get(0).start()
    loads[3].start()
    ring.barrier()
    loads[0].wait()
    g = Gather(ring, buf, send, recv)
    pending = []

    def compute(chip):
        s = len(pending)
        if s == 0:
            loads[1].wait()
        at = rows_at(chip * (2 * rows), 2 * rows)
        keep = pltpu.make_async_copy(buf.at[at], full_ref.at[at], store.at[s])
        keep.start()
        stage[s] = dot_nt(w_s[...], buf[at, :]).astype(jnp.bfloat16)
        out = pltpu.make_async_copy(stage.at[s], out_ref.at[:, at], put.at[s])
        out.start()
        pending.append((keep, out))

    def fill(k):
        mid = up.total // 2
        if k == 0:
            loads[2].wait()
            up.run(0, mid)
        elif k == 1:
            up.run(mid, up.total)
            loads[3].wait()
            down.run(0, down.total // 2)
        else:
            down.run(down.total // 2, down.total)

    g.run(compute, fill)
    up.finish()
    down.finish()
    for pair in pending:
        for cp in pair:
            cp.wait()


def gather_grads(n, cid, x, w, b1, dz, g, dy, unit=256):
    rows, hidden = x.shape
    seq, m, chips, ffn = rows * n, w.shape[0], n // 2, dz.shape[1]
    dma = pltpu.SemaphoreType.DMA
    shape = lambda *d: jax.ShapeDtypeStruct(d, x.dtype)
    vmem = lambda *d: pltpu.VMEM(d, x.dtype)
    return pl.pallas_call(
        functools.partial(gather_grads_kernel, n),
        in_specs=[pl.BlockSpec(memory_space=pl.ANY)] * 6,
        out_specs=[pl.BlockSpec(memory_space=pl.ANY)] * 4,
        out_shape=[shape(seq, hidden), shape(m, seq), shape(hidden, ffn), shape(ffn, hidden)],
        scratch_shapes=[vmem(seq, hidden), vmem(*w.shape), vmem(chips, m, 2 * rows), vmem(seq, ffn), vmem(seq, hidden),
                        vmem(2, seq, unit), vmem(2, seq, unit), vmem(unit, seq), vmem(2, unit, ffn), vmem(2, unit, hidden),
                        dma((13,)), dma((13,)), dma((4,)), dma((chips,)), dma((chips,)),
                        dma((2,)), dma((2,)), dma((2,)), dma((2,))],
        compiler_params=pltpu.CompilerParams(collective_id=cid, has_side_effects=True, vmem_limit_bytes=60 * 2 ** 20),
        cost_estimate=pl.CostEstimate(flops=60 * 10 ** 9, bytes_accessed=6 * seq * hidden, transcendentals=0),
        name="gather_grads",
    )(x, w, b1, dz, g, dy)


def add_rows(dst, start, count, *terms, cols=slice(None)):
    step = 32

    def body(i, c):
        at = rows_at(start + i * step, step)
        total = dst[at, cols].astype(jnp.float32)
        for ref, first in terms:
            total = total + ref[rows_at(first + i * step, step), cols].astype(jnp.float32)
        dst[at, cols] = total.astype(jnp.bfloat16)
        return c

    lax.fori_loop(0, count // step, body, 0)


class Scatter:
    def __init__(self, ring, part, pin, mid, fin, send, recv, tile=512):
        self.tiles, self.first_tiles = part.shape[2] // tile, 2
        cut = self.first_tiles * tile
        self.cols = {2: slice(0, cut), 4: slice(0, cut), 5: slice(0, cut)}
        self.cols.update({k: slice(cut, part.shape[2]) for k in (10, 11, 12)})
        self.ring, self.part, self.pin, self.mid, self.fin, self.send, self.recv = ring, part, pin, mid, fin, send, recv
        self.rows = part.shape[1] // 2
        self.half = self.rows // 2
        self.own = ring.core * self.rows

    def copy(self, k):
        r, h = self.ring, self.half
        cols = self.cols.get(k)
        if k in (2, 10):
            src, dst, dev = self.part.at[2, rows_at((1 - r.core) * self.rows, self.rows), cols], self.pin.at[2, :, cols], r.partner
        elif k in (4, 11):
            src, dst, dev = self.part.at[2, rows_at(self.own, h), cols], self.mid.at[0, :, cols], r.next
        elif k in (5, 12):
            src, dst, dev = self.part.at[2, rows_at(self.own + h, h), cols], self.mid.at[1, :, cols], r.prev
        elif k < 4:
            src, dst, dev = self.part.at[k, rows_at((1 - r.core) * self.rows, self.rows)], self.pin.at[k], r.partner
        else:
            d, half, dst, dev = {6: (1, 1, self.fin.at[0, h:], r.next), 7: (1, 0, self.fin.at[0, :h], r.next),
                                 8: (3, 0, self.fin.at[1, :h], r.prev), 9: (3, 1, self.fin.at[1, h:], r.prev)}[k]
            src = self.part.at[d, rows_at(self.own + half * h, h)]
        return pltpu.make_async_remote_copy(src_ref=src, dst_ref=dst, send_sem=self.send.at[k], recv_sem=self.recv.at[k],
                                            device_id={'model': dev}, device_id_type=MESH)

    def start(self, k):
        self.copy(k).start()

    def arrived(self, k):
        self.copy(k).wait_recv()

    def join(self, d):
        self.arrived(d)
        add_rows(self.part.at[d], self.own, self.rows, (self.pin.at[d], 0))

    def run(self, product, filler, emit):
        h = self.half
        every = (0, self.tiles)
        for lo, hi, away, up, down in ((0, self.first_tiles, 2, 4, 5), (self.first_tiles, self.tiles, 10, 11, 12)):
            product(2, self.rows - self.own, self.rows, (lo, hi), True)
            self.start(away)
            product(2, self.own, self.rows, (lo, hi), False)
            self.arrived(away)
            add_rows(self.part.at[2], self.own, self.rows, (self.pin.at[2], 0), cols=self.cols[away])
            self.start(up)
            self.start(down)
        for d in (1, 3):
            product(d, 0, 2 * self.rows, every, False)
            self.start(d)
        self.join(1)
        self.start(6)
        self.join(3)
        self.start(8)
        product(0, 0, 2 * self.rows, every, False)
        self.start(0)
        self.arrived(4)
        self.arrived(11)
        add_rows(self.part.at[1], self.own, h, (self.mid.at[0], 0))
        self.start(7)
        self.arrived(5)
        self.arrived(12)
        add_rows(self.part.at[3], self.own + h, h, (self.mid.at[1], 0))
        self.start(9)
        self.join(0)
        filler()
        for k in (6, 7, 8, 9):
            self.arrived(k)
        step = 16

        def body(i, c):
            at = rows_at(i * step, step)
            total = self.part[0, rows_at(self.own + i * step, step), :].astype(jnp.float32)
            total = total + self.fin[0, at, :].astype(jnp.float32) + self.fin[1, at, :].astype(jnp.float32)
            emit(at, total.astype(jnp.bfloat16))
            return c

        lax.fori_loop(0, self.rows // step, body, 0)
        for k in range(13):
            self.copy(k).wait_send()


def normalized(x):
    mean = jnp.mean(x, axis=-1, keepdims=True)
    cen = x - mean
    rstd = lax.rsqrt(jnp.mean(cen * cen, axis=-1, keepdims=True) + LN_EPS)
    return cen * rstd, rstd


def prepare_norm(x_s, hat_s, rstd_s):
    step = 16

    def body(i, c):
        at = rows_at(i * step, step)
        hat, rstd = normalized(x_s[at, :].astype(jnp.float32))
        hat_s[at, :] = hat
        rstd_s[at, :] = jnp.broadcast_to(rstd, (step, rstd_s.shape[1]))
        return c

    lax.fori_loop(0, x_s.shape[0] // step, body, 0)


def norm_scratch(rows, hidden):
    return [pltpu.VMEM((rows, hidden), jnp.float32), pltpu.VMEM((rows, 128), jnp.float32)]


def norm_backward(hat, rstd, gain, d):
    dh = d * gain
    return rstd * (dh - jnp.mean(dh, axis=-1, keepdims=True) - hat * jnp.mean(dh * hat, axis=-1, keepdims=True))


def fold_rows(v):
    return v[:8, :] + v[8:, :]


class Weights:
    def __init__(self, src, dst, sem, tile, rows):
        self.src, self.dst, self.sem, self.tile, self.rows = src, dst, sem, tile, rows
        self.count = src.shape[0 if rows else 1] // tile

    def copy(self, t):
        at = rows_at(t * self.tile, self.tile)
        if self.rows:
            return pltpu.make_async_copy(self.src.at[at], self.dst.at[at], self.sem.at[t])
        return pltpu.make_async_copy(self.src.at[:, at], self.dst.at[:, at], self.sem.at[t])

    def start(self):
        for t in range(self.count):
            self.copy(t).start()


def product_t(ring, tile, x_s, weights, lhs, part):
    wide = part.shape[1]

    def product(d, row0, count, tiles, first):
        if (first and tiles[0] == 0) or d != 2:
            lhs[...] = x_s[:, rows_at(ring.ahead(d) * wide, wide)].T
        at = rows_at(row0, count)

        def body(t, c):
            cols = rows_at(t * tile, tile)
            if first:
                weights.copy(t).wait()
            part[d, at, cols] = dot32(lhs[at, :], weights.dst[:, cols]).astype(jnp.bfloat16)
            return c

        lax.fori_loop(tiles[0], tiles[1], body, 0)

    return product


def scatter_scratch(rows, hidden, dtype):
    dma = pltpu.SemaphoreType.DMA
    return [pltpu.VMEM((4, 2 * rows, hidden), dtype), pltpu.VMEM((4, rows, hidden), dtype),
            pltpu.VMEM((2, rows // 2, hidden), dtype), pltpu.VMEM((2, rows, hidden), dtype), dma((13,)), dma((13,))]


def scatter_norm_kernel(n, tile, x_ref, w_ref, res_ref, gain_ref, mid_ref, norm_ref,
                        x_s, w_s, lhs, res_s, part, pin, mid, fin, send, recv, load, wl):
    ring = Ring(n)
    loads = [pltpu.make_async_copy(a, b, load.at[i]) for i, (a, b) in enumerate(((x_ref, x_s), (res_ref, res_s)))]
    weights = Weights(w_ref, w_s, wl, tile, False)
    loads[0].start()
    weights.start()
    loads[1].start()
    ring.barrier()
    loads[0].wait()
    sc = Scatter(ring, part, pin, mid, fin, send, recv)

    def emit(at, total):
        x1 = (res_s[at, :].astype(jnp.float32) + total.astype(jnp.float32)).astype(jnp.bfloat16)
        mid_ref[at, :] = x1
        norm_ref[at, :] = (normalized(x1.astype(jnp.float32))[0] * gain_ref[...]).astype(jnp.bfloat16)

    sc.run(product_t(ring, tile, x_s, weights, lhs, part), lambda: loads[1].wait(), emit)


def scatter_norm(n, cid, x, w, res, gain, tile=512):
    (m, seq), hidden = x.shape, w.shape[1]
    rows = seq // n
    dma = pltpu.SemaphoreType.DMA
    vmem = lambda *d: pltpu.VMEM(d, x.dtype)
    any_spec, vm = pl.BlockSpec(memory_space=pl.ANY), pl.BlockSpec(memory_space=pltpu.VMEM)
    return pl.pallas_call(
        functools.partial(scatter_norm_kernel, n, tile),
        in_specs=[any_spec] * 3 + [vm],
        out_specs=[vm] * 2,
        out_shape=[jax.ShapeDtypeStruct((rows, hidden), x.dtype)] * 2,
        scratch_shapes=[vmem(*x.shape), vmem(*w.shape), vmem(2 * rows, m), vmem(rows, hidden)]
        + scatter_scratch(rows, hidden, x.dtype) + [dma((2,)), dma((hidden // tile,))],
        compiler_params=pltpu.CompilerParams(collective_id=cid, has_side_effects=True, vmem_limit_bytes=60 * 2 ** 20),
        cost_estimate=pl.CostEstimate(flops=40 * 10 ** 9, bytes_accessed=3 * seq * hidden, transcendentals=0),
        name="scatter_norm",
    )(x, w, res, gain)


def scatter_grads_kernel(n, tile, x_ref, w_ref, a_ref, o_ref, d_ref, res_ref, dmid_ref, gain_ref, dg2_ref,
                         out_ref, gq_ref, go_ref, sums_ref,
                         x_s, w_s, lhs, o_s, a_s, d_s, gq_st, go_st, res_s, dmid_s, acc, mine, slots, hat_s, rstd_s,
                         part, pin, mid, fin, send, recv, load, wl, a_l, a_p, d_l, d_p, gsend, grecv):
    ring = Ring(n)
    peers = [lax.rem(ring.me + k, n) for k in range(1, n)]
    loads = [pltpu.make_async_copy(a, b, load.at[i]) for i, (a, b) in
             enumerate(((x_ref, x_s), (o_ref, o_s), (res_ref, res_s), (dmid_ref, dmid_s)))]
    weights = Weights(w_ref, w_s, wl, tile, False)
    loads[0].start()
    weights.start()
    wq = Product(a_ref, x_s, gq_ref, a_s, gq_st, a_l, a_p, False)
    wo = Product(d_ref, o_s, go_ref, d_s, go_st, d_l, d_p, False)
    ring.barrier(peers)
    for cp in loads[1:]:
        cp.start()
    wq.get(0).start()
    wo.get(0).start()
    loads[0].wait()
    sc = Scatter(ring, part, pin, mid, fin, send, recv)
    acc[...] = jnp.zeros_like(acc)

    def filler():
        loads[1].wait()
        wq.run(0, wq.total)
        wo.run(0, wo.total)
        loads[2].wait()
        loads[3].wait()
        prepare_norm(res_s, hat_s, rstd_s)

    def emit(at, total):
        out_ref[at, :] = total
        acc[...] += fold_rows(total.astype(jnp.float32) * hat_s[at, :])

    sc.run(product_t(ring, tile, x_s, weights, lhs, part), filler, emit)
    mine[0:1, :] = jnp.sum(acc[...], axis=0, keepdims=True)
    mine[1:2, :] = dg2_ref[...]
    step = 16

    def body(i, c):
        at = rows_at(i * step, step)
        dx = norm_backward(hat_s[at, :], rstd_s[at, 0:1], gain_ref[...], out_ref[at, :].astype(jnp.float32))
        out_ref[at, :] = (dmid_s[at, :].astype(jnp.float32) + dx).astype(jnp.bfloat16)
        return c

    steps = out_ref.shape[0] // step
    lax.fori_loop(0, steps // 4, body, 0)
    copies = [pltpu.make_async_remote_copy(src_ref=mine, dst_ref=slots.at[ring.me], send_sem=gsend.at[k], recv_sem=grecv.at[k],
                                           device_id={'model': dev}, device_id_type=MESH) for k, dev in enumerate(peers)]
    for cp in copies:
        cp.start()
    slots[ring.me] = mine[...]
    lax.fori_loop(steps // 4, steps, body, 0)
    wq.finish()
    wo.finish()
    for cp in copies:
        cp.wait()
    total = slots[0]
    for k in range(1, n):
        total = total + slots[k]
    sums_ref[...] = total.astype(jnp.bfloat16)


def scatter_grads(n, cid, x, w, a, o, d, res, d_mid, gain, dg2, tile=512):
    (m, seq), hidden = x.shape, w.shape[1]
    rows = seq // n
    dma = pltpu.SemaphoreType.DMA
    vmem = lambda *s: pltpu.VMEM(s, x.dtype)
    any_spec, vm = pl.BlockSpec(memory_space=pl.ANY), pl.BlockSpec(memory_space=pltpu.VMEM)
    return pl.pallas_call(
        functools.partial(scatter_grads_kernel, n, tile),
        in_specs=[any_spec] * 7 + [vm] * 2,
        out_specs=[vm, any_spec, any_spec, vm],
        out_shape=[jax.ShapeDtypeStruct((rows, hidden), x.dtype), jax.ShapeDtypeStruct(w.shape, x.dtype),
                   jax.ShapeDtypeStruct((o.shape[0], hidden), x.dtype), jax.ShapeDtypeStruct((2, hidden), x.dtype)],
        scratch_shapes=[vmem(*x.shape), vmem(*w.shape), vmem(2 * rows, m), vmem(*o.shape), vmem(2, seq, tile), vmem(2, seq, tile),
                        vmem(2, m, tile), vmem(2, o.shape[0], tile), vmem(rows, hidden), vmem(rows, hidden),
                        pltpu.VMEM((8, hidden), jnp.float32), pltpu.VMEM((2, hidden), jnp.float32),
                        pltpu.VMEM((n, 2, hidden), jnp.float32)] + norm_scratch(rows, hidden)
        + scatter_scratch(rows, hidden, x.dtype)
        + [dma((4,)), dma((hidden // tile,)), dma((2,)), dma((2,)), dma((2,)), dma((2,)), dma((n - 1,)), dma((n - 1,))],
        compiler_params=pltpu.CompilerParams(collective_id=cid, has_side_effects=True, vmem_limit_bytes=63 * 2 ** 20),
        cost_estimate=pl.CostEstimate(flops=60 * 10 ** 9, bytes_accessed=6 * seq * hidden, transcendentals=0),
        name="scatter_grads",
    )(x, w, a, o, d, res, d_mid, gain, dg2)


def scatter_mlp_kernel(n, tile, dz_ref, up_ref, g_ref, down_ref, res_ref, dy_ref, gain_ref, out_ref, y_ref, dg_ref,
                       dz_s, w_s, g_s, down_s, res_s, dy_s, acc, hat_s, rstd_s, part, pin, mid, fin, send, recv, load, wl, zl, ystage, put):
    ring = Ring(n)
    loads = [pltpu.make_async_copy(a, b, load.at[i]) for i, (a, b) in
             enumerate(((res_ref, res_s), (dy_ref, dy_s), (g_ref, g_s), (down_ref, down_s)))]
    wide = part.shape[1]
    hidden = part.shape[2]

    def dz_at(d):
        return rows_at(ring.ahead(d) * wide, wide)

    dz_loads = [pltpu.make_async_copy(dz_ref.at[dz_at(d)], dz_s.at[dz_at(d)], zl.at[d]) for d in range(4)]
    weights = Weights(up_ref, w_s, wl, tile, True)
    dz_loads[2].start()
    weights.start()
    ring.barrier()
    for d in (1, 3, 0):
        dz_loads[d].start()
    sc = Scatter(ring, part, pin, mid, fin, send, recv)
    acc[...] = jnp.zeros_like(acc)

    def product(d, row0, count, tiles, first):
        if (first and tiles[0] == 0) or d != 2:
            dz_loads[d].wait()
        if d == 3:
            for cp in loads:
                cp.start()
        src = rows_at(ring.ahead(d) * wide + row0, count, 256)
        at = rows_at(row0, count, 256)

        def body(t, c):
            cols = rows_at(t * tile, tile)
            if first:
                weights.copy(t).wait()
            part[d, at, cols] = dot_nt(dz_s[src, :], w_s[cols, :]).astype(jnp.bfloat16)
            return c

        lax.fori_loop(tiles[0], tiles[1], body, 0)

    def emit(at, total):
        d = total.astype(jnp.float32)
        hat = hat_s[at, :]
        dx = norm_backward(hat, rstd_s[at, 0:1], gain_ref[...], d)
        out_ref[at, :] = (dy_s[at, :].astype(jnp.float32) + dx).astype(jnp.bfloat16)
        acc[...] += fold_rows(d * hat)

    def filler():
        for cp in loads:
            cp.wait()
        puts = []
        for q in range(n // 2):
            if q >= 2:
                puts[q - 2].wait()

            def body(t, c):
                cols = rows_at(t * tile, tile)
                ystage[q % 2, :, cols] = dot32(g_s[q * wide:(q + 1) * wide, :], down_s[:, cols]).astype(jnp.bfloat16)
                return c

            lax.fori_loop(0, hidden // tile, body, 0)
            puts.append(pltpu.make_async_copy(ystage.at[q % 2], y_ref.at[q * wide:(q + 1) * wide], put.at[q]))
            puts[q].start()
        prepare_norm(res_s, hat_s, rstd_s)
        for cp in puts[-2:]:
            cp.wait()

    sc.run(product, filler, emit)
    dg_ref[...] = jnp.sum(acc[...], axis=0, keepdims=True)


def scatter_mlp(n, cid, dz, up, g, down, res, dy, gain, tile=512):
    (seq, ffn), hidden = dz.shape, down.shape[1]
    rows = seq // n
    dma = pltpu.SemaphoreType.DMA
    any_spec, vm = pl.BlockSpec(memory_space=pl.ANY), pl.BlockSpec(memory_space=pltpu.VMEM)
    return pl.pallas_call(
        functools.partial(scatter_mlp_kernel, n, tile),
        in_specs=[any_spec] * 6 + [vm],
        out_specs=[vm, any_spec, vm],
        out_shape=[jax.ShapeDtypeStruct((rows, hidden), dz.dtype), jax.ShapeDtypeStruct((seq, hidden), dz.dtype),
                   jax.ShapeDtypeStruct((1, hidden), jnp.float32)],
        scratch_shapes=[pltpu.VMEM(a.shape, a.dtype) for a in (dz, up, g, down, res, dy)]
        + [pltpu.VMEM((8, hidden), jnp.float32)] + norm_scratch(rows, hidden) + scatter_scratch(rows, hidden, dz.dtype)
        + [dma((4,)), dma((hidden // tile,)), dma((4,)), pltpu.VMEM((2, 2 * rows, hidden), dz.dtype), dma((n // 2,))],
        compiler_params=pltpu.CompilerParams(collective_id=cid, has_side_effects=True, vmem_limit_bytes=63 * 2 ** 20),
        cost_estimate=pl.CostEstimate(flops=60 * 10 ** 9, bytes_accessed=3 * seq * hidden, transcendentals=0),
        name="scatter_mlp",
    )(dz, up, g, down, res, dy, gain)


def local_layer(n, hidden_in, seg_ids, gain_attn, w_qkv, w_out, gain_mlp, w_up, w_down, grad_out):
    heads, hd, hidden = w_out.shape
    seq_len = seg_ids.shape[1]
    x_f32 = hidden_in[0].astype(jnp.float32)
    dy = grad_out[0]
    wq_t = jnp.transpose(w_qkv, (1, 2, 3, 0)).reshape(heads * 3 * hd, hidden)
    wo = w_out.reshape(heads * hd, hidden)
    first = jnp.sum(seg_ids[0][:, None] < seg_ids[0][None, :], axis=0, dtype=jnp.int32)
    lo = first[::BLK] // BLK
    first = first[None]
    gather = lambda a: lax.all_gather(a, 'model', axis=0, tiled=True)
    scatter = lambda a: lax.psum_scatter(a, 'model', scatter_dimension=0, tiled=True)

    gain1 = gain_attn.astype(jnp.float32)
    gain2 = gain_mlp.astype(jnp.float32)[None]
    attn_in, qkv_t = gather_t(n, 0, layer_norm(x_f32, gain1).astype(jnp.bfloat16), wq_t, 320)
    dy_late, qkv_t = lax.optimization_barrier((dy, qkv_t))
    grad_full = gather(dy_late)
    o_t, lse = attention_fwd(qkv_t, lo, first, heads, hd)
    mid_loc, norm2 = scatter_norm(n, 1, o_t, wo, hidden_in[0], gain2)
    mlp_in, act_lo, d_pre = mlp(n, 2, norm2, grad_full, w_up, w_down)
    d_mid, mlp_part, d_gain_mlp = scatter_mlp(n, 3, d_pre, w_up, act_lo, w_down, mid_loc, dy, gain2)
    d_mid_full, do_t, g_up, g_down = gather_grads(n, 4, d_mid, wo, mlp_in, d_pre, act_lo, grad_full)
    mlp_part, do_t = lax.optimization_barrier((mlp_part, do_t))
    mlp_sum = scatter(mlp_part)
    hidden_out = (mid_loc.astype(jnp.float32) + mlp_sum.astype(jnp.float32)).astype(jnp.bfloat16)
    dqkv_t, g_up, g_down = attention_bwd(qkv_t, o_t, do_t, lse, lo, first, g_up, g_down, heads, hd)
    grad_in, g_qkv, g_out, gain_sums = scatter_grads(n, 5, dqkv_t, wq_t, attn_in, o_t, d_mid_full, hidden_in[0], d_mid,
                                                     gain1[None], d_gain_mlp)
    g_qkv = jnp.transpose(g_qkv.reshape(heads, 3, hd, hidden), (3, 0, 1, 2))
    return (hidden_out[None], grad_in[None], g_qkv, g_out.reshape(heads, hd, hidden), g_up, g_down,
            gain_sums[0], gain_sums[1])


def solution(mesh):
    act_spec = P('data', 'model', None)
    in_specs = (act_spec, P('data', None), P(), P(None, 'model', None, None), P('model', None, None), P(), P(None, 'model'), P('model', None), act_spec)
    out_specs = (act_spec, act_spec, P('data', 'model', None, None), P(('data', 'model'), None, None), P('data', 'model'), P(('data', 'model'), None), P('data'), P('data'))
    return jax.shard_map(functools.partial(local_layer, mesh.shape['model']), mesh=mesh, in_specs=in_specs, out_specs=out_specs, check_vma=False)
```
